128 devices in a mesh: data: 1, dap: 128 (over z, y, x, core).
Axes of the slice: x: 4, y: 4, z: 4, core: 2. Of those that a mesh axis runs over, the one named last changes fastest.
Arguments:
- msa_act: bfloat16 [2048, 512, 256], P(('data', 'dap'))
- msa_mask: int32 [2048, 512], P(('data', 'dap'))
- pair_act: float32 [512, 512, 128], P(('data', 'dap'))
- opm_gain: bfloat16 [256], replicated
- opm_shift: bfloat16 [256], replicated
- proj_a: bfloat16 [256, 32], replicated
- bias_a: bfloat16 [32], replicated
- proj_b: bfloat16 [256, 32], replicated
- bias_b: bfloat16 [32], replicated
- proj_out: bfloat16 [1024, 128], replicated
- bias_out: bfloat16 [128], replicated
- row_gain: bfloat16 [256], replicated
- row_shift: bfloat16 [256], replicated
- pair_gain: bfloat16 [128], replicated
- pair_proj: bfloat16 [128, 8], replicated
- query_w: bfloat16 [256, 256], replicated
- key_w: bfloat16 [256, 256], replicated
- value_w: bfloat16 [256, 256], replicated
- gate_w: bfloat16 [256, 256], replicated
- gate_bias: bfloat16 [256], replicated
- attn_out_w: bfloat16 [256, 256], replicated
- attn_out_b: bfloat16 [256], replicated
Outputs:
- output 1: bfloat16 [2048, 512, 256], P(('data', 'dap'))
- output 2: float32 [512, 512, 128], P(('data', 'dap'))
All inputs are finite; a program needn't handle non-finite values.
Results may differ from the reference program's by a relative error of at most 0.00800763.
Values are sent between devices in bfloat16 or wider.
A program may use at most 1 GiB of HBM per device.

```python
import math
import jax
import jax.numpy as jnp
from jax import lax

S = 2048
N = 512
CM = 256
CZ = 128
CH = 32
HEADS = 8
HEAD = 32
SEQ_BLOCK = math.gcd(S, 8)
BLOCK_COUNT = S // SEQ_BLOCK


def gauss_draw(draw_key, arr_shape, std_scale):
    return jax.random.normal(draw_key, arr_shape, jnp.float32) * std_scale


def draw_mask(draw_key):
    seq_key, res_key, elem_key = jax.random.split(draw_key, 3)
    seq_dens = jax.random.randint(seq_key, (S, 1), 0, 17)
    res_dens = jax.random.randint(res_key, (1, N), 8, 17)
    draws = jax.random.randint(elem_key, (S, N), 0, 256)
    kept = (draws < seq_dens * res_dens).astype(jnp.int32)
    query_row = (jnp.arange(S) == 0)[:, None]
    return jnp.where(query_row, 1, kept).astype(jnp.int32)


def setup_inputs(seed: int = 0, part: int = 0) -> dict:
    part_keys = jax.random.split(jax.random.fold_in(jax.random.key(seed), part), 3)
    weight_keys = jax.random.split(jax.random.key(seed + 1), 19)
    bias_scale = 0.8 * S ** -0.25
    shift_scale = 0.5 * S ** -0.25
    head_total = HEADS * HEAD
    return dict(
        msa_act=gauss_draw(part_keys[0], (S, N, CM), 0.25).astype(jnp.bfloat16),
        msa_mask=draw_mask(part_keys[1]),
        pair_act=gauss_draw(part_keys[2], (N, N, CZ), 2.0 * S ** -0.5),
        opm_gain=(1.0 + gauss_draw(weight_keys[0], (CM,), 0.3)).astype(jnp.bfloat16),
        opm_shift=gauss_draw(weight_keys[1], (CM,), shift_scale).astype(jnp.bfloat16),
        proj_a=gauss_draw(weight_keys[2], (CM, CH), CM ** -0.5).astype(jnp.bfloat16),
        bias_a=gauss_draw(weight_keys[3], (CH,), bias_scale).astype(jnp.bfloat16),
        proj_b=gauss_draw(weight_keys[4], (CM, CH), CM ** -0.5).astype(jnp.bfloat16),
        bias_b=gauss_draw(weight_keys[5], (CH,), bias_scale).astype(jnp.bfloat16),
        proj_out=gauss_draw(weight_keys[6], (CH * CH, CZ), 1.0 / CH).astype(jnp.bfloat16),
        bias_out=gauss_draw(weight_keys[7], (CZ,), 0.3 * S ** 0.5).astype(jnp.bfloat16),
        row_gain=(1.0 + gauss_draw(weight_keys[8], (CM,), 0.3)).astype(jnp.bfloat16),
        row_shift=gauss_draw(weight_keys[9], (CM,), 0.3).astype(jnp.bfloat16),
        pair_gain=(1.0 + gauss_draw(weight_keys[10], (CZ,), 0.3)).astype(jnp.bfloat16),
        pair_proj=gauss_draw(weight_keys[11], (CZ, HEADS), CZ ** -0.5).astype(jnp.bfloat16),
        query_w=gauss_draw(weight_keys[12], (CM, head_total), CM ** -0.5).astype(jnp.bfloat16),
        key_w=gauss_draw(weight_keys[13], (CM, head_total), CM ** -0.5).astype(jnp.bfloat16),
        value_w=gauss_draw(weight_keys[14], (CM, head_total), CM ** -0.5).astype(jnp.bfloat16),
        gate_w=gauss_draw(weight_keys[15], (CM, head_total), CM ** -0.5).astype(jnp.bfloat16),
        gate_bias=gauss_draw(weight_keys[16], (head_total,), 1.0).astype(jnp.bfloat16),
        attn_out_w=gauss_draw(weight_keys[17], (head_total, CM), head_total ** -0.5).astype(jnp.bfloat16),
        attn_out_b=gauss_draw(weight_keys[18], (CM,), 0.1).astype(jnp.bfloat16),
    )


def layer_norm(values, norm_gain):
    values = values.astype(jnp.float32)
    centered = values - jnp.mean(values, axis=-1, keepdims=True)
    variance = jnp.mean(jnp.square(centered), axis=-1, keepdims=True)
    return centered * lax.rsqrt(variance + 1e-5) * norm_gain.astype(jnp.float32)


def project(values, weight):
    lead_shape = values.shape[:-1]
    flat_out = jnp.dot(values.reshape(-1, values.shape[-1]), weight, preferred_element_type=jnp.float32)
    return flat_out.reshape(lead_shape + (weight.shape[-1],))


def reference(msa_act, msa_mask, pair_act, opm_gain, opm_shift, proj_a, bias_a, proj_b, bias_b, proj_out, bias_out, row_gain, row_shift, pair_gain, pair_proj, query_w, key_w, value_w, gate_w, gate_bias, attn_out_w, attn_out_b):
    mask_val = msa_mask.astype(jnp.float32)
    proj_cube = proj_out.reshape(CH, CH, CZ).astype(jnp.float32)
    msa_blocks = msa_act.reshape(BLOCK_COUNT, SEQ_BLOCK, N, CM)
    mask_blocks = mask_val.reshape(BLOCK_COUNT, SEQ_BLOCK, N)

    def opm_step(outer_acc, blk_in):
        msa_blk, mask_blk = blk_in
        normed = (layer_norm(msa_blk, opm_gain) + opm_shift.astype(jnp.float32)).astype(jnp.bfloat16)
        left_act = ((project(normed, proj_a) + bias_a.astype(jnp.float32)) * mask_blk[:, :, None]).astype(jnp.bfloat16)
        right_act = ((project(normed, proj_b) + bias_b.astype(jnp.float32)) * mask_blk[:, :, None]).astype(jnp.bfloat16)
        left_proj = jnp.einsum('sic,cde->side', left_act.astype(jnp.float32), proj_cube).astype(jnp.bfloat16)
        outer_acc = outer_acc + jnp.einsum('side,sjd->ije', left_proj.astype(jnp.float32), right_act.astype(jnp.float32))
        return outer_acc, None

    outer_sum, _ = lax.scan(opm_step, jnp.zeros((N, N, CZ), jnp.float32), (msa_blocks, mask_blocks))
    counts = jnp.dot(mask_val.T, mask_val, preferred_element_type=jnp.float32)
    pair_out = pair_act + (outer_sum + bias_out.astype(jnp.float32)) / (1e-3 + counts)[:, :, None]

    pair_normed = layer_norm(pair_act, pair_gain).astype(jnp.bfloat16)
    pair_bias = jnp.einsum('ije,eh->hij', pair_normed.astype(jnp.float32), pair_proj.astype(jnp.float32)).astype(jnp.bfloat16).astype(jnp.float32)
    heads_shape = (SEQ_BLOCK, N, HEADS, HEAD)

    def attend(blk_in):
        msa_blk, mask_blk = blk_in
        normed = (layer_norm(msa_blk, row_gain) + row_shift.astype(jnp.float32)).astype(jnp.bfloat16)
        query_act = project(normed, query_w).astype(jnp.bfloat16).reshape(heads_shape)
        key_act = project(normed, key_w).astype(jnp.bfloat16).reshape(heads_shape)
        value_act = project(normed, value_w).astype(jnp.bfloat16).reshape(heads_shape)
        gate_act = jax.nn.sigmoid(project(normed, gate_w) + gate_bias.astype(jnp.float32)).astype(jnp.bfloat16).reshape(heads_shape)
        logits = jnp.einsum('sihd,sjhd->shij', query_act.astype(jnp.float32), key_act.astype(jnp.float32)) * (HEAD ** -0.5) + pair_bias[None]
        logits = jnp.where(mask_blk[:, None, None, :] > 0, logits, -1e9)
        weights = jax.nn.softmax(logits, axis=-1).astype(jnp.bfloat16)
        attended = jnp.einsum('shij,sjhd->sihd', weights.astype(jnp.float32), value_act.astype(jnp.float32))
        gated = (attended * gate_act.astype(jnp.float32)).astype(jnp.bfloat16).reshape(SEQ_BLOCK, N, HEADS * HEAD)
        update = project(gated, attn_out_w) + attn_out_b.astype(jnp.float32)
        return (msa_blk.astype(jnp.float32) + update).astype(jnp.bfloat16)

    msa_out = lax.map(attend, (msa_blocks, mask_blocks)).reshape(S, N, CM)
    return (msa_out, pair_out)
```

```python
import functools
import math
import jax
import jax.numpy as jnp
from jax import lax
from jax.experimental import pallas as pl
from jax.experimental.pallas import tpu as pltpu
from jax.sharding import Mesh, PartitionSpec as P

LN_EPS = 1e-5
COUNT_EPS = 1e-3
MASK_FILL = -1e9
VMEM_LIMIT = 60 * 1024 * 1024
GROUP_AXES = ('z', 'y')
SPLIT_AXES = ('x', 'c')


def attn_kernel(chunk, msa_ref, mask_ref, bias_ref, gain_ref, shift_ref, w_ref, gb_ref, wo_ref, bo_ref, out_ref, q_scr, k_scr, vb_scr, g_scr, w_scr):
    n, cm = msa_ref.shape[1:]
    heads = bias_ref.shape[0]
    hd = cm // heads
    x = msa_ref[0].astype(jnp.float32)
    mu = jnp.mean(x, axis=-1, keepdims=True)
    xc = x - mu
    var = jnp.mean(xc * xc, axis=-1, keepdims=True)
    r = (xc * lax.rsqrt(var + LN_EPS) * gain_ref[...].astype(jnp.float32) + shift_ref[...].astype(jnp.float32)).astype(jnp.bfloat16)
    q_scr[...] = jnp.dot(r, w_ref[:, 0:cm], preferred_element_type=jnp.float32).astype(jnp.bfloat16)
    k_scr[...] = jnp.dot(r, w_ref[:, cm:2*cm], preferred_element_type=jnp.float32).astype(jnp.bfloat16)
    v = jnp.dot(r, w_ref[:, 2*cm:3*cm], preferred_element_type=jnp.float32).astype(jnp.bfloat16)
    g_scr[...] = jax.nn.sigmoid(jnp.dot(r, w_ref[:, 3*cm:4*cm], preferred_element_type=jnp.float32) + gb_ref[...].astype(jnp.float32)).astype(jnp.bfloat16)
    lane_head = lax.broadcasted_iota(jnp.int32, (1, cm), 1) // hd
    for h in range(heads):
        vb_scr[h*n:(h+1)*n, :] = v * (lane_head == h).astype(jnp.bfloat16)
    keep = mask_ref[0] > 0
    scale = hd ** -0.5

    def rows(ci, carry):
        r0 = pl.multiple_of(ci * chunk, chunk)
        qc = q_scr[pl.ds(r0, chunk), :]
        for h in range(heads):
            qh = qc * (lane_head == h).astype(jnp.bfloat16)
            s = lax.dot_general(qh, k_scr[...], (((1,), (1,)), ((), ())), preferred_element_type=jnp.float32)
            s = s * scale + bias_ref[h, pl.ds(r0, chunk), :]
            s = jnp.where(keep, s, MASK_FILL)
            m = jnp.max(s, axis=-1, keepdims=True)
            e = jnp.exp(s - m)
            l = jnp.sum(e, axis=-1, keepdims=True)
            w_scr[:, h*n:(h+1)*n] = (e * (1.0 / l)).astype(jnp.bfloat16)
        o = jnp.dot(w_scr[...], vb_scr[...], preferred_element_type=jnp.float32)
        o = (o * g_scr[pl.ds(r0, chunk), :].astype(jnp.float32)).astype(jnp.bfloat16)
        u = jnp.dot(o, wo_ref[...], preferred_element_type=jnp.float32) + bo_ref[...].astype(jnp.float32)
        out_ref[0, pl.ds(r0, chunk), :] = (msa_ref[0, pl.ds(r0, chunk), :].astype(jnp.float32) + u).astype(jnp.bfloat16)
        return carry
    lax.fori_loop(0, n // chunk, rows, 0)

def attention(msa, mask, bias, gain, shift, wqkvg, gb, wo, bo, chunk=512):
    s, n, cm = msa.shape
    heads = bias.shape[0]
    const = lambda shape: pl.BlockSpec(shape, lambda i: (0,)*len(shape), pipeline_mode=pl.Buffered(1))
    return pl.pallas_call(
        functools.partial(attn_kernel, chunk),
        out_shape=jax.ShapeDtypeStruct((s, n, cm), jnp.bfloat16),
        grid=(s,),
        in_specs=[pl.BlockSpec((1, n, cm), lambda i: (i, 0, 0)), pl.BlockSpec((1, 1, n), lambda i: (i, 0, 0)),
                  const((heads, n, n)), const((1, cm)), const((1, cm)), const((cm, 4*cm)), const((1, cm)), const((cm, cm)), const((1, cm))],
        out_specs=pl.BlockSpec((1, n, cm), lambda i: (i, 0, 0)),
        scratch_shapes=[pltpu.VMEM((n, cm), jnp.bfloat16), pltpu.VMEM((n, cm), jnp.bfloat16), pltpu.VMEM((heads*n, cm), jnp.bfloat16),
                        pltpu.VMEM((n, cm), jnp.bfloat16), pltpu.VMEM((chunk, heads*n), jnp.bfloat16)],
        compiler_params=pltpu.CompilerParams(vmem_limit_bytes=60*1024*1024, dimension_semantics=("arbitrary",)),
        cost_estimate=pl.CostEstimate(flops=16*1000000000, bytes_accessed=20_000_000, transcendentals=33_000_000),
        name="row_attention",
    )(msa, mask, bias, gain, shift, wqkvg, gb, wo, bo)


def ab_kernel(msa_ref, mask_ref, gain_ref, shift_ref, w_ref, bias_ref, a_ref, b_ref, scr):
    seqs, n, cm = msa_ref.shape
    ch = a_ref.shape[0]

    def one(s, carry):
        x = msa_ref[s].astype(jnp.float32)
        mu = jnp.mean(x, axis=-1, keepdims=True)
        xc = x - mu
        var = jnp.mean(xc * xc, axis=-1, keepdims=True)
        xn = (xc * lax.rsqrt(var + LN_EPS) * gain_ref[...].astype(jnp.float32) + shift_ref[...].astype(jnp.float32)).astype(jnp.bfloat16)
        y = lax.dot_general(w_ref[...], xn, (((1,), (1,)), ((), ())), preferred_element_type=jnp.float32)
        y = (y + bias_ref[...]) * mask_ref[s]
        scr[:, pl.ds(s, 1), :] = y.reshape(2 * ch, 1, n)
        return carry
    lax.fori_loop(0, seqs, one, 0)
    a_ref[...] = scr[0:ch].astype(jnp.bfloat16)
    b_ref[0:ch] = scr[ch:2 * ch].astype(jnp.bfloat16)
    b_ref[ch] = mask_ref[:, 0, :].astype(jnp.bfloat16)


def project_ab(msa, mask, gain, shift, w_t, bias_t):
    s, n, cm = msa.shape
    ch = w_t.shape[0] // 2
    return pl.pallas_call(
        ab_kernel,
        out_shape=(jax.ShapeDtypeStruct((ch, s, n), jnp.bfloat16), jax.ShapeDtypeStruct((ch + 1, s, n), jnp.bfloat16)),
        scratch_shapes=[pltpu.VMEM((2 * ch, s, n), jnp.float32)],
        compiler_params=pltpu.CompilerParams(vmem_limit_bytes=VMEM_LIMIT),
        cost_estimate=pl.CostEstimate(flops=300_000_000, bytes_accessed=6_000_000, transcendentals=8192),
        name="project_ab",
    )(msa, mask, gain, shift, w_t, bias_t)


def opm_kernel(db, ib, at_ref, pt_ref, b_ref, m_ref, sel_ref, out_ref, lhs):
    rows = out_ref.shape[0]
    ce = pt_ref.shape[0] // db
    k = at_ref.shape[1] // rows
    n = out_ref.shape[2]
    step = pl.program_id(0)

    @pl.when(step == 0)
    def _():
        m = m_ref[...].reshape(k, n)
        mi = lax.dot_general(sel_ref[...], m, (((1,), (1,)), ((), ())), preferred_element_type=jnp.float32).astype(jnp.bfloat16)
        cnt = jnp.dot(mi, m, preferred_element_type=jnp.float32)
        for i in range(rows):
            out_ref[i, 0:ce, :] = jnp.zeros((ce, n), jnp.float32)
            out_ref[i, ce:, :] = jnp.broadcast_to(cnt[i:i + 1, :], (out_ref.shape[1] - ce, n))

    bk = jnp.concatenate([b_ref[:, dd].reshape(k, n) for dd in range(db)], axis=0)

    def block(g, carry):
        for ii in range(ib):
            col = pl.multiple_of((g * ib + ii) * k, k)
            ai = at_ref[:, pl.ds(col, k)]
            for dd in range(db):
                u = jnp.dot(pt_ref[dd * ce:(dd + 1) * ce, :], ai, preferred_element_type=jnp.float32)
                lhs[ii * ce:(ii + 1) * ce, dd * k:(dd + 1) * k] = u.astype(jnp.bfloat16)
        part = jnp.dot(lhs[...], bk, preferred_element_type=jnp.float32)
        for ii in range(ib):
            out_ref[g * ib + ii, 0:ce, :] += part[ii * ce:(ii + 1) * ce]
        return carry
    lax.fori_loop(0, rows // ib, block, 0)


def outer_product(a_t, p_t, b_all, sel, rows, db=4, ib=8):
    ch, cols = a_t.shape
    src, _, s, n = b_all.shape
    ce = p_t.shape[0] // ch
    k = src * s
    return pl.pallas_call(
        functools.partial(opm_kernel, db, ib),
        out_shape=jax.ShapeDtypeStruct((rows, ce + 8, n), jnp.float32),
        grid=(ch // db,),
        in_specs=[pl.BlockSpec((ch, cols), lambda g: (0, 0)),
                  pl.BlockSpec((db * ce, ch), lambda g: (g, 0)),
                  pl.BlockSpec((src, db, s, n), lambda g: (0, g, 0, 0)),
                  pl.BlockSpec((src, 1, s, n), lambda g: (0, ch, 0, 0)),
                  pl.BlockSpec((rows, n), lambda g: (0, 0))],
        out_specs=pl.BlockSpec((rows, ce + 8, n), lambda g: (0, 0, 0)),
        scratch_shapes=[pltpu.VMEM((ib * ce, db * k), jnp.bfloat16)],
        compiler_params=pltpu.CompilerParams(vmem_limit_bytes=VMEM_LIMIT, dimension_semantics=("arbitrary",)),
        cost_estimate=pl.CostEstimate(flops=2 * rows * ce * n * k * ch, bytes_accessed=20_000_000, transcendentals=0),
        name="outer_product",
    )(a_t, p_t, b_all, b_all, sel)


def solution(mesh):
    devices = mesh.devices
    fine = Mesh(devices.reshape(devices.shape[0], 4, 4, 4, 2), ('data', 'z', 'y', 'x', 'c'))
    everyone = ('z', 'y', 'x', 'c')
    seq_spec = P(('data',) + everyone)

    def per_device(msa, msa_mask, pair_act, opm_gain, opm_shift, proj_a, bias_a, proj_b, bias_b, proj_out, bias_out, row_gain, row_shift, pair_gain, pair_proj, query_w, key_w, value_w, gate_w, gate_bias, attn_out_w, attn_out_b):
        seqs, n, cm = msa.shape
        rows_dev, _, ce = pair_act.shape
        ch = proj_a.shape[1]
        groups = fine.shape['z'] * fine.shape['y']
        rows = n // groups
        mask = msa_mask.astype(jnp.float32).reshape(seqs, 1, n)

        pair_c = pair_act - jnp.mean(pair_act, axis=-1, keepdims=True)
        pair_var = jnp.mean(jnp.square(pair_c), axis=-1, keepdims=True)
        pair_n = (pair_c * lax.rsqrt(pair_var + LN_EPS) * pair_gain.astype(jnp.float32)).astype(jnp.bfloat16)
        bias_rows = jnp.einsum('ije,eh->ihj', pair_n, pair_proj, preferred_element_type=jnp.float32).astype(jnp.bfloat16)

        w_t = jnp.concatenate([proj_a, proj_b], axis=1).T
        ab_bias = jnp.concatenate([bias_a, bias_b]).astype(jnp.float32)[:, None]
        a_loc, b_loc = project_ab(msa, mask, opm_gain[None], opm_shift[None], w_t, ab_bias)
        b_all = lax.all_gather(b_loc, GROUP_AXES, axis=0, tiled=False)
        bias_all = lax.all_gather(bias_rows, everyone, axis=0, tiled=True)
        pair_bias = bias_all.transpose(1, 0, 2).astype(jnp.float32)

        a_send = a_loc.reshape(ch, seqs, groups, rows).transpose(2, 0, 1, 3).reshape(groups, ch, seqs * rows)
        a_recv = lax.all_to_all(a_send, GROUP_AXES, 0, 0, tiled=True)
        a_t = a_recv.reshape(groups, ch, seqs, rows).transpose(1, 3, 0, 2).reshape(ch, rows * groups * seqs)
        p_t = proj_out.reshape(ch, ch, ce).transpose(1, 2, 0).reshape(ch * ce, ch)
        first = lax.axis_index(GROUP_AXES) * rows
        sel = (lax.broadcasted_iota(jnp.int32, (rows, n), 1) == lax.broadcasted_iota(jnp.int32, (rows, n), 0) + first).astype(jnp.bfloat16)
        part = outer_product(a_t, p_t, b_all, sel, rows)
        total = lax.psum_scatter(part, SPLIT_AXES, scatter_dimension=0, tiled=True)
        outer_sum = total[:, :ce].transpose(0, 2, 1)
        counts = total[:, ce]
        pair_new = pair_act + (outer_sum + bias_out.astype(jnp.float32)) / (COUNT_EPS + counts)[:, :, None]

        qkvg_w = jnp.concatenate([query_w, key_w, value_w, gate_w], axis=1)
        msa_new = attention(msa, mask, pair_bias, row_gain[None], row_shift[None], qkvg_w, gate_bias[None], attn_out_w, attn_out_b[None])
        return msa_new, pair_new

    in_specs = (seq_spec, seq_spec, seq_spec) + (P(),) * 19
    return jax.shard_map(per_device, mesh=fine, in_specs=in_specs, out_specs=(seq_spec, seq_spec), check_vma=False)
```

```python
import functools
import math
import jax
import jax.numpy as jnp
from jax import lax
from jax.experimental import pallas as pl
from jax.experimental.pallas import tpu as pltpu
from jax.sharding import Mesh, PartitionSpec as P

LN_EPS = 1e-5
COUNT_EPS = 1e-3
MASK_FILL = -1e9
VMEM_LIMIT = 60 * 1024 * 1024
LANES = 128
SUBLANES = 8
ALL_AXES = ('z', 'y', 'x', 'c')
GROUP_AXES = ('z', 'y')
SPLIT_AXES = ('x', 'c')


def attn_kernel(chunk, msa_ref, mask_ref, bias_ref, gain_ref, shift_ref, w_ref, gb_ref, wo_ref, bo_ref, *rest):
    out_ref, q_scr, k_scr, vb_scr, g_scr, w_scr = rest[-6:]
    n, cm = msa_ref.shape[1:]
    heads = bias_ref.shape[0]
    hd = cm // heads
    x = msa_ref[0].astype(jnp.float32)
    mu = jnp.mean(x, axis=-1, keepdims=True)
    xc = x - mu
    var = jnp.mean(xc * xc, axis=-1, keepdims=True)
    r = (xc * lax.rsqrt(var + LN_EPS) * gain_ref[...].astype(jnp.float32) + shift_ref[...].astype(jnp.float32)).astype(jnp.bfloat16)
    q_scr[...] = jnp.dot(r, w_ref[:, 0:cm], preferred_element_type=jnp.float32).astype(jnp.bfloat16)
    k_scr[...] = jnp.dot(r, w_ref[:, cm:2*cm], preferred_element_type=jnp.float32).astype(jnp.bfloat16)
    v = jnp.dot(r, w_ref[:, 2*cm:3*cm], preferred_element_type=jnp.float32).astype(jnp.bfloat16)
    g_scr[...] = jax.nn.sigmoid(jnp.dot(r, w_ref[:, 3*cm:4*cm], preferred_element_type=jnp.float32) + gb_ref[...].astype(jnp.float32)).astype(jnp.bfloat16)
    lane_head = lax.broadcasted_iota(jnp.int32, (1, cm), 1) // hd
    for h in range(heads):
        vb_scr[h*n:(h+1)*n, :] = v * (lane_head == h).astype(jnp.bfloat16)
    keep = mask_ref[0] > 0
    scale = hd ** -0.5

    def rows(ci, carry):
        r0 = pl.multiple_of(ci * chunk, chunk)
        qc = q_scr[pl.ds(r0, chunk), :]
        for h in range(heads):
            qh = qc * (lane_head == h).astype(jnp.bfloat16)
            s = lax.dot_general(qh, k_scr[...], (((1,), (1,)), ((), ())), preferred_element_type=jnp.float32)
            s = s * scale + bias_ref[h, pl.ds(r0, chunk), :]
            s = jnp.where(keep, s, MASK_FILL)
            m = jnp.max(s, axis=-1, keepdims=True)
            e = jnp.exp(s - m)
            l = jnp.sum(e, axis=-1, keepdims=True)
            w_scr[:, h*n:(h+1)*n] = (e * (1.0 / l)).astype(jnp.bfloat16)
        o = jnp.dot(w_scr[...], vb_scr[...], preferred_element_type=jnp.float32)
        o = (o * g_scr[pl.ds(r0, chunk), :].astype(jnp.float32)).astype(jnp.bfloat16)
        u = jnp.dot(o, wo_ref[...], preferred_element_type=jnp.float32) + bo_ref[...].astype(jnp.float32)
        out_ref[0, pl.ds(r0, chunk), :] = (msa_ref[0, pl.ds(r0, chunk), :].astype(jnp.float32) + u).astype(jnp.bfloat16)
        return carry
    lax.fori_loop(0, n // chunk, rows, 0)

def attention(msa, mask, bias, gain, shift, wqkvg, gb, wo, bo, first, count, before=None, chunk=512):
    s, n, cm = msa.shape
    heads = bias.shape[0]
    const = lambda shape: pl.BlockSpec(shape, lambda i: (0,) * len(shape), pipeline_mode=pl.Buffered(1))
    extra = () if before is None else (before,)
    return pl.pallas_call(
        functools.partial(attn_kernel, chunk),
        out_shape=jax.ShapeDtypeStruct((s, n, cm), jnp.bfloat16),
        grid=(count,),
        in_specs=[pl.BlockSpec((1, n, cm), lambda i: (i + first, 0, 0)), pl.BlockSpec((1, 1, n), lambda i: (i + first, 0, 0)),
                  const((heads, n, n)), const((1, cm)), const((1, cm)), const((cm, 4 * cm)), const((1, cm)), const((cm, cm)), const((1, cm))]
                 + [pl.BlockSpec(memory_space=pl.ANY)] * len(extra),
        out_specs=pl.BlockSpec((1, n, cm), lambda i: (i + first, 0, 0)),
        scratch_shapes=[pltpu.VMEM((n, cm), jnp.bfloat16), pltpu.VMEM((n, cm), jnp.bfloat16), pltpu.VMEM((heads * n, cm), jnp.bfloat16),
                        pltpu.VMEM((n, cm), jnp.bfloat16), pltpu.VMEM((chunk, heads * n), jnp.bfloat16)],
        input_output_aliases={9: 0} if extra else {},
        compiler_params=pltpu.CompilerParams(vmem_limit_bytes=VMEM_LIMIT, dimension_semantics=("arbitrary",)),
        cost_estimate=pl.CostEstimate(flops=count * 1_500_000_000, bytes_accessed=20_000_000, transcendentals=count * 2_000_000),
        name="row_attention",
    )(msa, mask, bias, gain, shift, wqkvg, gb, wo, bo, *extra)


def ab_kernel(msa_ref, mask_ref, gain_ref, shift_ref, w_ref, bias_ref, a_ref, b_ref, scr_a, scr_b):
    seqs, n, cm = msa_ref.shape
    ch = scr_b.shape[0]
    quads = n // LANES
    subs = a_ref.shape[0] // quads
    width = LANES // subs
    lane = lax.broadcasted_iota(jnp.int32, (SUBLANES, LANES), 1) // width

    def one(s, carry):
        x = msa_ref[s].astype(jnp.float32)
        mu = jnp.mean(x, axis=-1, keepdims=True)
        xc = x - mu
        var = jnp.mean(xc * xc, axis=-1, keepdims=True)
        xn = (xc * lax.rsqrt(var + LN_EPS) * gain_ref[...].astype(jnp.float32) + shift_ref[...].astype(jnp.float32)).astype(jnp.bfloat16)
        y = lax.dot_general(w_ref[...], xn, (((1,), (1,)), ((), ())), preferred_element_type=jnp.float32)
        y = (y + bias_ref[...]) * mask_ref[s]
        scr_b[:, pl.ds(s, 1), :] = y[ch:2 * ch].reshape(ch, 1, n)
        for zz in range(quads):
            tiles = [y[c4 * SUBLANES:(c4 + 1) * SUBLANES, zz * LANES:(zz + 1) * LANES] for c4 in range(subs)]
            for yy in range(subs):
                out = tiles[yy]
                for c4 in range(subs):
                    if c4 != yy:
                        out = jnp.where(lane == c4, pltpu.roll(tiles[c4], ((c4 - yy) * width) % LANES, 1), out)
                scr_a[zz * subs + yy, pl.ds(pl.multiple_of(s * SUBLANES, SUBLANES), SUBLANES), :] = out
        return carry
    lax.fori_loop(0, seqs, one, 0)
    a_ref[...] = scr_a[...].astype(jnp.bfloat16)
    b_ref[0:ch] = scr_b[...].astype(jnp.bfloat16)
    b_ref[ch] = mask_ref[:, 0, :].astype(jnp.bfloat16)


def project_ab(msa, mask, gain, shift, w_t, bias_t):
    s, n, cm = msa.shape
    ch = w_t.shape[0] // 2
    return pl.pallas_call(
        ab_kernel,
        out_shape=(jax.ShapeDtypeStruct((16, s * SUBLANES, LANES), jnp.bfloat16), jax.ShapeDtypeStruct((ch + 1, s, n), jnp.bfloat16)),
        scratch_shapes=[pltpu.VMEM((16, s * SUBLANES, LANES), jnp.float32), pltpu.VMEM((ch, s, n), jnp.float32)],
        compiler_params=pltpu.CompilerParams(vmem_limit_bytes=VMEM_LIMIT),
        cost_estimate=pl.CostEstimate(flops=300_000_000, bytes_accessed=6_000_000, transcendentals=8192),
        name="project_ab",
    )(msa, mask, gain, shift, w_t, bias_t)


def opm_kernel(db, ib, half, ar_ref, pt_ref, b_ref, m_ref, sel_ref, out_ref, lhs, af, at2):
    rows = out_ref.shape[0]
    ce = pt_ref.shape[0] // db
    ch = pt_ref.shape[1]
    k = m_ref.shape[0] * m_ref.shape[2]
    n = out_ref.shape[2]
    full = at2.shape[1] // ch
    step = pl.program_id(0)

    @pl.when(step == 0)
    def _():
        m = m_ref[...].reshape(k, n)
        mi = lax.dot_general(sel_ref[...], m, (((1,), (1,)), ((), ())), preferred_element_type=jnp.float32).astype(jnp.bfloat16)
        cnt = jnp.dot(mi, m, preferred_element_type=jnp.float32)
        for i in range(rows):
            out_ref[i, 0:ce, :] = jnp.zeros((ce, n), jnp.float32)
            out_ref[i, ce:, :] = jnp.broadcast_to(cnt[i:i + 1, :], (out_ref.shape[1] - ce, n))
        af[...] = ar_ref[...].reshape(af.shape).astype(jnp.float32)
        eye = (lax.broadcasted_iota(jnp.int32, (LANES, LANES), 0) == lax.broadcasted_iota(jnp.int32, (LANES, LANES), 1)).astype(jnp.bfloat16)
        for c8 in range(SUBLANES):
            x = af[pl.ds(c8, k, stride=SUBLANES), :].astype(jnp.bfloat16)
            t = lax.dot_general(eye, x, (((1,), (1,)), ((), ())), preferred_element_type=jnp.float32)
            for c4 in range(ch // SUBLANES):
                for kk in range(k // LANES):
                    at2[kk, pl.ds(c4 * SUBLANES + c8, full, stride=ch), :] = t[c4 * full:(c4 + 1) * full, kk * LANES:(kk + 1) * LANES]

    bk = jnp.concatenate([b_ref[:, dd].reshape(k, n) for dd in range(db)], axis=0)

    def block(g, carry):
        for ii in range(ib):
            i = (g * (ib // 2) + ii // 2) * 4 + half * 2 + ii % 2
            ai = jnp.concatenate([at2[kk, pl.ds(pl.multiple_of(i * ch, ch), ch), :] for kk in range(k // LANES)], axis=1).astype(jnp.bfloat16)
            for dd in range(db):
                u = jnp.dot(pt_ref[dd * ce:(dd + 1) * ce, :], ai, preferred_element_type=jnp.float32)
                lhs[ii * ce:(ii + 1) * ce, dd * k:(dd + 1) * k] = u.astype(jnp.bfloat16)
        part = jnp.dot(lhs[...], bk, preferred_element_type=jnp.float32)
        for ii in range(ib):
            out_ref[g * ib + ii, 0:ce, :] += part[ii * ce:(ii + 1) * ce]
        return carry
    lax.fori_loop(0, rows // ib, block, 0)


def outer_product(a_recv, p_t, b_all, sel, half, db=4, ib=8):
    rows = sel.shape[0]
    ch = p_t.shape[1]
    src, _, s, n = b_all.shape
    ce = p_t.shape[0] // ch
    k = src * s
    return pl.pallas_call(
        functools.partial(opm_kernel, db, ib, half),
        out_shape=jax.ShapeDtypeStruct((rows, ce + 8, n), jnp.float32),
        grid=(ch // db,),
        in_specs=[pl.BlockSpec(a_recv.shape, lambda g: (0, 0, 0)),
                  pl.BlockSpec((db * ce, ch), lambda g: (g, 0)),
                  pl.BlockSpec((src, db, s, n), lambda g: (0, g, 0, 0)),
                  pl.BlockSpec((src, 1, s, n), lambda g: (0, ch, 0, 0)),
                  pl.BlockSpec((rows, n), lambda g: (0, 0))],
        out_specs=pl.BlockSpec((rows, ce + 8, n), lambda g: (0, 0, 0)),
        scratch_shapes=[pltpu.VMEM((ib * ce, db * k), jnp.bfloat16), pltpu.VMEM((k * SUBLANES, LANES), jnp.float32),
                        pltpu.VMEM((k // LANES, 2 * rows * ch, LANES), jnp.float32)],
        compiler_params=pltpu.CompilerParams(vmem_limit_bytes=VMEM_LIMIT, dimension_semantics=("arbitrary",)),
        cost_estimate=pl.CostEstimate(flops=2 * rows * ce * n * k * ch, bytes_accessed=20_000_000, transcendentals=0),
        name="outer_product",
    )(a_recv, p_t, b_all, b_all, sel)


def exchange_kernel(rows_ref, a_ref, bias_ref, ar_ref, own_sem, send_sem, recv_sem, a_send, a_recv):
    mesh_id = pl.DeviceIdType.MESH
    me = {name: lax.axis_index(name) for name in ALL_AXES}
    size = {'z': bias_ref.shape[1], 'y': bias_ref.shape[2], 'x': bias_ref.shape[3], 'c': bias_ref.shape[4]}

    def moved(name, k):
        return lax.rem(me[name] + k, size[name])

    plane = [(dz, dy) for dz in range(size['z']) for dy in range(size['y']) if dz or dy]
    barrier = pltpu.get_barrier_semaphore()
    peers = [{'z': moved('z', dz), 'y': moved('y', dy)} for dz, dy in plane]
    peers += [{'x': moved('x', k)} for k in range(1, size['x'])] + [{'c': moved('c', k)} for k in range(1, size['c'])]
    for peer in peers:
        pl.semaphore_signal(barrier, inc=1, device_id=peer, device_id_type=mesh_id)

    own = [pltpu.make_async_copy(rows_ref.at[part], bias_ref.at[part, me['z'], me['y'], me['x'], me['c']], own_sem.at[part]) for part in range(2)]
    for copy in own:
        copy.start()
    pl.semaphore_wait(barrier, len(peers))

    def spread(part, name, done, slot):
        where = tuple(pl.ds(0, size[ax]) if ax in done else me[ax] for ax in ALL_AXES)
        ref = bias_ref.at[(part,) + where]
        copies = []
        for k in range(1, size[name]):
            copies.append(pltpu.make_async_remote_copy(
                src_ref=ref, dst_ref=ref, send_sem=send_sem.at[slot, k - 1], recv_sem=recv_sem.at[slot, k - 1],
                device_id={name: moved(name, k)}, device_id_type=mesh_id))
        for copy in copies:
            copy.start()
        return copies

    for copy in own:
        copy.wait()
    orders = (('x', 'y', 'z'), ('z', 'x', 'y'))
    flying = [spread(part, orders[part][0], (), part) for part in range(2)]
    here = me['z'] * size['y'] + me['y']
    sends = []
    for j, (dz, dy) in enumerate(plane):
        dst = moved('z', dz) * size['y'] + moved('y', dy)
        sends.append(pltpu.make_async_remote_copy(
            src_ref=a_ref.at[dst], dst_ref=ar_ref.at[here], send_sem=a_send.at[j], recv_sem=a_recv.at[j],
            device_id={'z': moved('z', dz), 'y': moved('y', dy)}, device_id_type=mesh_id))
    for copy in sends:
        copy.start()
    ar_ref[here] = a_ref[here]
    for phase in range(1, 3):
        for part in range(2):
            for copy in flying[part]:
                copy.wait()
            flying[part] = spread(part, orders[part][phase], orders[part][:phase], phase * 2 + part)
    for part in range(2):
        for copy in flying[part]:
            copy.wait()
        flying[part] = spread(part, 'c', orders[part], 6 + part)
    for copy in flying[0] + flying[1] + sends:
        copy.wait()


def exchange(rows, a_msg, sizes):
    half = rows.shape[1:]
    hops = max(sizes) - 1
    groups = sizes[0] * sizes[1]
    return pl.pallas_call(
        exchange_kernel,
        out_shape=(jax.ShapeDtypeStruct((2,) + tuple(sizes) + half, jnp.bfloat16), jax.ShapeDtypeStruct(a_msg.shape, jnp.bfloat16)),
        in_specs=[pl.BlockSpec(memory_space=pl.ANY), pl.BlockSpec(memory_space=pltpu.VMEM)],
        out_specs=(pl.BlockSpec(memory_space=pltpu.VMEM), pl.BlockSpec(memory_space=pltpu.VMEM)),
        scratch_shapes=[pltpu.SemaphoreType.DMA((2,)), pltpu.SemaphoreType.DMA((8, hops)), pltpu.SemaphoreType.DMA((8, hops)),
                        pltpu.SemaphoreType.DMA((groups - 1,)), pltpu.SemaphoreType.DMA((groups - 1,))],
        compiler_params=pltpu.CompilerParams(collective_id=0, has_side_effects=True, vmem_limit_bytes=VMEM_LIMIT),
        cost_estimate=pl.CostEstimate(flops=10_000_000_000, bytes_accessed=10_000_000, transcendentals=0),
        name="exchange",
    )(rows, a_msg)


def solution(mesh):
    devices = mesh.devices
    fine = Mesh(devices.reshape(devices.shape[0], 4, 4, 4, 2), ('data', 'z', 'y', 'x', 'c'))
    seq_spec = P(('data',) + ALL_AXES)

    def per_device(msa, msa_mask, pair_act, opm_gain, opm_shift, proj_a, bias_a, proj_b, bias_b, proj_out, bias_out, row_gain, row_shift, pair_gain, pair_proj, query_w, key_w, value_w, gate_w, gate_bias, attn_out_w, attn_out_b):
        seqs, n, cm = msa.shape
        rows_dev, _, ce = pair_act.shape
        ch = proj_a.shape[1]
        groups = fine.shape['z'] * fine.shape['y']
        rows = n // groups
        mask = msa_mask.astype(jnp.float32).reshape(seqs, 1, n)

        w_t = jnp.concatenate([proj_a, proj_b], axis=1).T
        ab_bias = jnp.concatenate([bias_a, bias_b]).astype(jnp.float32)[:, None]
        a_msg, b_loc = project_ab(msa, mask, opm_gain[None], opm_shift[None], w_t, ab_bias)
        b_all = lax.all_gather(b_loc, GROUP_AXES, axis=0, tiled=False)

        pair_in, a_msg = lax.optimization_barrier((pair_act, a_msg))
        pair_c = pair_in - jnp.mean(pair_in, axis=-1, keepdims=True)
        pair_var = jnp.mean(jnp.square(pair_c), axis=-1, keepdims=True)
        pair_n = (pair_c * lax.rsqrt(pair_var + LN_EPS) * pair_gain.astype(jnp.float32)).astype(jnp.bfloat16)
        bias_rows = jnp.einsum('ije,eh->ihj', pair_n, pair_proj, preferred_element_type=jnp.float32).astype(jnp.bfloat16)
        heads = bias_rows.shape[1]
        bias_rows = bias_rows.reshape(rows_dev, heads, 2, n // 2).transpose(2, 0, 1, 3).reshape(2, rows_dev * heads, n // 2)
        sizes = tuple(fine.shape[ax] for ax in ALL_AXES)
        bias_all, a_recv = exchange(bias_rows, a_msg, sizes)
        pair_bias = bias_all.reshape(2, n, heads, n // 2).transpose(2, 1, 0, 3).reshape(heads, n, n).astype(jnp.float32)

        qkvg_w = jnp.concatenate([query_w, key_w, value_w, gate_w], axis=1)
        attend = functools.partial(attention, msa, mask, pair_bias, row_gain[None], row_shift[None], qkvg_w, gate_bias[None], attn_out_w, attn_out_b[None])
        early = seqs // 2
        msa_new = attend(0, early)
        a_recv, msa_new = lax.optimization_barrier((a_recv, msa_new))

        p_t = proj_out.reshape(ch, ch, ce).transpose(1, 2, 0).reshape(ch * ce, ch)
        first = lax.axis_index(GROUP_AXES) * rows
        order = lax.broadcasted_iota(jnp.int32, (rows // 2, n), 0)
        cols = lax.broadcasted_iota(jnp.int32, (rows // 2, n), 1)
        totals = []
        for half in range(2):
            mine = first + (order // 2) * 4 + half * 2 + order % 2
            part = outer_product(a_recv, p_t, b_all, (cols == mine).astype(jnp.bfloat16), half)
            totals.append(lax.psum_scatter(part, SPLIT_AXES, scatter_dimension=0, tiled=True))
        msa_new, _ = lax.optimization_barrier((msa_new, part))
        msa_new = attend(early, seqs - early, msa_new)
        total = jnp.concatenate(totals, axis=0)
        outer_sum = total[:, :ce].transpose(0, 2, 1)
        counts = total[:, ce]
        pair_new = pair_act + (outer_sum + bias_out.astype(jnp.float32)) / (COUNT_EPS + counts)[:, :, None]
        return msa_new, pair_new

    in_specs = (seq_spec, seq_spec, seq_spec) + (P(),) * 19
    return jax.shard_map(per_device, mesh=fine, in_specs=in_specs, out_specs=(seq_spec, seq_spec), check_vma=False)
```

```python
import functools
import math
import jax
import jax.numpy as jnp
from jax import lax
from jax.experimental import pallas as pl
from jax.experimental.pallas import tpu as pltpu
from jax.sharding import Mesh, PartitionSpec as P

LN_EPS = 1e-5
COUNT_EPS = 1e-3
MASK_FILL = -1e9
LOG2E = math.log2(math.e)
VMEM_LIMIT = 60 * 1024 * 1024
LANES = 128
SUBLANES = 8
ALL_AXES = ('z', 'y', 'x', 'c')
GROUP_AXES = ('z', 'y')
SPLIT_AXES = ('x', 'c')


def attn_kernel(first, msa_ref, mask_ref, bias_ref, gain_ref, shift_ref, qw_ref, kw_ref, vw_ref, gw_ref, gb_ref, wo_ref, bo_ref, *rest):
    out_ref, q_scr, k_scr, v_scr, g_scr, w_scr, vb_scr = rest[-7:]
    n, cm = msa_ref.shape[1:]
    heads = bias_ref.shape[0]
    hd = cm // heads
    near, rest_scale = split_scale(hd)
    x = msa_ref[0].astype(jnp.float32)
    mu = jnp.mean(x, axis=-1, keepdims=True)
    xc = x - mu
    var = jnp.mean(xc * xc, axis=-1, keepdims=True)
    r = (xc * lax.rsqrt(var + LN_EPS) * gain_ref[...].astype(jnp.float32) + shift_ref[...].astype(jnp.float32)).astype(jnp.bfloat16)
    q_scr[...] = jnp.dot(r, qw_ref[...], preferred_element_type=jnp.float32).astype(jnp.bfloat16) * jnp.bfloat16(near)
    k_scr[...] = jnp.dot(r, kw_ref[...], preferred_element_type=jnp.float32).astype(jnp.bfloat16)
    v = jnp.dot(r, vw_ref[...], preferred_element_type=jnp.float32).astype(jnp.bfloat16)
    g_scr[...] = jax.nn.sigmoid(jnp.dot(r, gw_ref[...], preferred_element_type=jnp.float32) + gb_ref[...].astype(jnp.float32)).astype(jnp.bfloat16)
    lane_head = lax.broadcasted_iota(jnp.int32, (1, cm), 1) // hd
    for h in range(heads):
        vb_scr[h * n:(h + 1) * n, :] = v * (lane_head == h).astype(jnp.bfloat16)
    keep = mask_ref[pl.ds(pl.program_id(0) + first, 1), :] > 0
    q = q_scr[...]
    for h in range(heads):
        qh = q * (lane_head == h).astype(jnp.bfloat16)
        s = lax.dot_general(qh, k_scr[...], (((1,), (1,)), ((), ())), preferred_element_type=jnp.float32)
        s = jnp.where(keep, s + bias_ref[h], MASK_FILL / rest_scale)
        m = jnp.max(s, axis=-1, keepdims=True)
        e = jnp.exp2((s - m) * (rest_scale * LOG2E))
        l = jnp.sum(e, axis=-1, keepdims=True)
        w_scr[:, h * n:(h + 1) * n] = (e * (1.0 / l)).astype(jnp.bfloat16)
    o = jnp.dot(w_scr[...], vb_scr[...], preferred_element_type=jnp.float32)
    o = (o * g_scr[...].astype(jnp.float32)).astype(jnp.bfloat16)
    u = jnp.dot(o, wo_ref[...], preferred_element_type=jnp.float32) + bo_ref[...].astype(jnp.float32)
    out_ref[0] = (msa_ref[0].astype(jnp.float32) + u).astype(jnp.bfloat16)


def split_scale(hd):
    near = 2.0 ** math.floor(math.log2(hd ** -0.5))
    return near, hd ** -0.5 / near


def attention(msa, mask, bias, gain, shift, qw, kw, vw, gw, gb, wo, bo, first, count, before=None):
    s, n, cm = msa.shape
    heads = bias.shape[0]
    const = lambda shape: pl.BlockSpec(shape, lambda i: (0,) * len(shape), pipeline_mode=pl.Buffered(1))
    extra = () if before is None else (before,)
    return pl.pallas_call(
        functools.partial(attn_kernel, first),
        out_shape=jax.ShapeDtypeStruct((s, n, cm), jnp.bfloat16),
        grid=(count,),
        in_specs=[pl.BlockSpec((1, n, cm), lambda i: (i + first, 0, 0)), const((s, n)),
                  const((heads, n, n)), const((1, cm)), const((1, cm)), const((cm, cm)), const((cm, cm)), const((cm, cm)), const((cm, cm)), const((1, cm)), const((cm, cm)), const((1, cm))]
                 + [pl.BlockSpec(memory_space=pl.ANY)] * len(extra),
        out_specs=pl.BlockSpec((1, n, cm), lambda i: (i + first, 0, 0)),
        scratch_shapes=[pltpu.VMEM((n, cm), jnp.bfloat16)] * 4 + [pltpu.VMEM((n, heads * n), jnp.bfloat16), pltpu.VMEM((heads * n, cm), jnp.bfloat16)],
        input_output_aliases={12: 0} if extra else {},
        compiler_params=pltpu.CompilerParams(vmem_limit_bytes=VMEM_LIMIT, dimension_semantics=("arbitrary",)),
        cost_estimate=pl.CostEstimate(flops=count * 1_500_000_000, bytes_accessed=20_000_000, transcendentals=count * 2_000_000),
        name="row_attention",
    )(msa, mask, bias, gain[None], shift[None], qw, kw, vw, gw, gb[None], wo, bo[None], *extra)


def ab_kernel(msa_ref, mask_ref, gain_ref, shift_ref, pa_ref, ba_ref, pb_ref, bb_ref, a_ref, b_ref, scr_a, scr_b):
    seqs, n, cm = msa_ref.shape
    ch = scr_b.shape[0]
    quads = n // LANES
    subs = a_ref.shape[0] // quads
    width = LANES // subs
    lane = lax.broadcasted_iota(jnp.int32, (SUBLANES, LANES), 1) // width
    w = jnp.concatenate([pa_ref[...], pb_ref[...]], axis=1).astype(jnp.float32).T.astype(jnp.bfloat16)
    bias = jnp.concatenate([ba_ref[...], bb_ref[...]], axis=1).astype(jnp.float32)
    bias = jnp.broadcast_to(bias, (SUBLANES, 2 * ch)).T[:, 0:1]
    gain = gain_ref[...].astype(jnp.float32)
    shift = shift_ref[...].astype(jnp.float32)

    def one(s, carry):
        x = msa_ref[s].astype(jnp.float32)
        mu = jnp.mean(x, axis=-1, keepdims=True)
        xc = x - mu
        var = jnp.mean(xc * xc, axis=-1, keepdims=True)
        xn = (xc * lax.rsqrt(var + LN_EPS) * gain + shift).astype(jnp.bfloat16)
        y = lax.dot_general(w, xn, (((1,), (1,)), ((), ())), preferred_element_type=jnp.float32)
        y = (y + bias) * mask_ref[pl.ds(s, 1), :].astype(jnp.float32)
        scr_b[:, pl.ds(s, 1), :] = y[ch:2 * ch].reshape(ch, 1, n)
        for zz in range(quads):
            tiles = [y[c4 * SUBLANES:(c4 + 1) * SUBLANES, zz * LANES:(zz + 1) * LANES] for c4 in range(subs)]
            for yy in range(subs):
                out = tiles[yy]
                for c4 in range(subs):
                    if c4 != yy:
                        out = jnp.where(lane == c4, pltpu.roll(tiles[c4], ((c4 - yy) * width) % LANES, 1), out)
                scr_a[zz * subs + yy, pl.ds(pl.multiple_of(s * SUBLANES, SUBLANES), SUBLANES), :] = out
        return carry
    lax.fori_loop(0, seqs, one, 0)
    a_ref[...] = scr_a[...].astype(jnp.bfloat16)
    b_ref[0:ch] = scr_b[...].astype(jnp.bfloat16)
    b_ref[ch] = mask_ref[...].astype(jnp.float32).astype(jnp.bfloat16)


def project_ab(msa, mask, gain, shift, proj_a, bias_a, proj_b, bias_b):
    s, n, cm = msa.shape
    ch = proj_a.shape[1]
    return pl.pallas_call(
        ab_kernel,
        out_shape=(jax.ShapeDtypeStruct((16, s * SUBLANES, LANES), jnp.bfloat16), jax.ShapeDtypeStruct((ch + 1, s, n), jnp.bfloat16)),
        scratch_shapes=[pltpu.VMEM((16, s * SUBLANES, LANES), jnp.float32), pltpu.VMEM((ch, s, n), jnp.float32)],
        compiler_params=pltpu.CompilerParams(vmem_limit_bytes=VMEM_LIMIT),
        cost_estimate=pl.CostEstimate(flops=300_000_000, bytes_accessed=6_000_000, transcendentals=8192),
        name="project_ab",
    )(msa, mask, gain[None], shift[None], proj_a, bias_a[None], proj_b, bias_b[None])


def opm_kernel(db, ib, half, ar_ref, pt_ref, b_ref, m_ref, sel_ref, out_ref, lhs, af, at2):
    rows = out_ref.shape[0]
    ce = pt_ref.shape[0] // db
    ch = pt_ref.shape[1]
    k = m_ref.shape[0] * m_ref.shape[2]
    n = out_ref.shape[2]
    full = at2.shape[1] // ch
    step = pl.program_id(0)

    @pl.when(step == 0)
    def _():
        m = m_ref[...].reshape(k, n)
        mi = lax.dot_general(sel_ref[...], m, (((1,), (1,)), ((), ())), preferred_element_type=jnp.float32).astype(jnp.bfloat16)
        cnt = jnp.dot(mi, m, preferred_element_type=jnp.float32)
        for i in range(rows):
            out_ref[i, 0:ce, :] = jnp.zeros((ce, n), jnp.float32)
            out_ref[i, ce:, :] = jnp.broadcast_to(cnt[i:i + 1, :], (out_ref.shape[1] - ce, n))
        af[...] = ar_ref[...].reshape(af.shape).astype(jnp.float32)
        eye = (lax.broadcasted_iota(jnp.int32, (LANES, LANES), 0) == lax.broadcasted_iota(jnp.int32, (LANES, LANES), 1)).astype(jnp.bfloat16)
        for c8 in range(SUBLANES):
            x = af[pl.ds(c8, k, stride=SUBLANES), :].astype(jnp.bfloat16)
            t = lax.dot_general(eye, x, (((1,), (1,)), ((), ())), preferred_element_type=jnp.float32)
            for c4 in range(ch // SUBLANES):
                for kk in range(k // LANES):
                    at2[kk, pl.ds(c4 * SUBLANES + c8, full, stride=ch), :] = t[c4 * full:(c4 + 1) * full, kk * LANES:(kk + 1) * LANES]

    bk = jnp.concatenate([b_ref[:, dd].reshape(k, n) for dd in range(db)], axis=0)

    def block(g, carry):
        for ii in range(ib):
            i = (g * (ib // 2) + ii // 2) * 4 + half * 2 + ii % 2
            ai = jnp.concatenate([at2[kk, pl.ds(pl.multiple_of(i * ch, ch), ch), :] for kk in range(k // LANES)], axis=1).astype(jnp.bfloat16)
            for dd in range(db):
                u = jnp.dot(pt_ref[dd * ce:(dd + 1) * ce, :], ai, preferred_element_type=jnp.float32)
                lhs[ii * ce:(ii + 1) * ce, dd * k:(dd + 1) * k] = u.astype(jnp.bfloat16)
        part = jnp.dot(lhs[...], bk, preferred_element_type=jnp.float32)
        for ii in range(ib):
            out_ref[g * ib + ii, 0:ce, :] += part[ii * ce:(ii + 1) * ce]
        return carry
    lax.fori_loop(0, rows // ib, block, 0)


def outer_product(a_recv, p_t, b_all, sel, half, db=4, ib=8):
    rows = sel.shape[0]
    ch = p_t.shape[1]
    src, _, s, n = b_all.shape
    ce = p_t.shape[0] // ch
    k = src * s
    return pl.pallas_call(
        functools.partial(opm_kernel, db, ib, half),
        out_shape=jax.ShapeDtypeStruct((rows, ce + 8, n), jnp.float32),
        grid=(ch // db,),
        in_specs=[pl.BlockSpec(a_recv.shape, lambda g: (0, 0, 0)),
                  pl.BlockSpec((db * ce, ch), lambda g: (g, 0)),
                  pl.BlockSpec((src, db, s, n), lambda g: (0, g, 0, 0)),
                  pl.BlockSpec((src, 1, s, n), lambda g: (0, ch, 0, 0)),
                  pl.BlockSpec((rows, n), lambda g: (0, 0))],
        out_specs=pl.BlockSpec((rows, ce + 8, n), lambda g: (0, 0, 0)),
        scratch_shapes=[pltpu.VMEM((ib * ce, db * k), jnp.bfloat16), pltpu.VMEM((k * SUBLANES, LANES), jnp.float32),
                        pltpu.VMEM((k // LANES, 2 * rows * ch, LANES), jnp.float32)],
        compiler_params=pltpu.CompilerParams(vmem_limit_bytes=VMEM_LIMIT, dimension_semantics=("arbitrary",)),
        cost_estimate=pl.CostEstimate(flops=2 * rows * ce * n * k * ch, bytes_accessed=20_000_000, transcendentals=0),
        name="outer_product",
    )(a_recv, p_t, b_all, b_all, sel)


def exchange_kernel(scale, rows_ref, a_ref, out_ref, ar_ref, bias_ref, tmp, own_sem, send_sem, recv_sem, a_send, a_recv):
    mesh_id = pl.DeviceIdType.MESH
    me = {name: lax.axis_index(name) for name in ALL_AXES}
    size = {'z': bias_ref.shape[1], 'y': bias_ref.shape[2], 'x': bias_ref.shape[3], 'c': bias_ref.shape[4]}

    def moved(name, k):
        return lax.rem(me[name] + k, size[name])

    plane = [(dz, dy) for dz in range(size['z']) for dy in range(size['y']) if dz or dy]
    barrier = pltpu.get_barrier_semaphore()
    peers = [{'z': moved('z', dz), 'y': moved('y', dy)} for dz, dy in plane]
    peers += [{'x': moved('x', k)} for k in range(1, size['x'])] + [{'c': moved('c', k)} for k in range(1, size['c'])]
    for peer in peers:
        pl.semaphore_signal(barrier, inc=1, device_id=peer, device_id_type=mesh_id)

    own = [pltpu.make_async_copy(rows_ref.at[part], bias_ref.at[part, me['z'], me['y'], me['x'], me['c']], own_sem.at[part]) for part in range(2)]
    for copy in own:
        copy.start()
    pl.semaphore_wait(barrier, len(peers))

    def spread(part, name, done, slot):
        where = tuple(pl.ds(0, size[ax]) if ax in done else me[ax] for ax in ALL_AXES)
        ref = bias_ref.at[(part,) + where]
        copies = []
        for k in range(1, size[name]):
            copies.append(pltpu.make_async_remote_copy(
                src_ref=ref, dst_ref=ref, send_sem=send_sem.at[slot, k - 1], recv_sem=recv_sem.at[slot, k - 1],
                device_id={name: moved(name, k)}, device_id_type=mesh_id))
        for copy in copies:
            copy.start()
        return copies

    for copy in own:
        copy.wait()
    orders = (('x', 'y', 'z'), ('z', 'x', 'y'))
    flying = [spread(part, orders[part][0], (), part) for part in range(2)]
    here = me['z'] * size['y'] + me['y']
    sends = []
    for j, (dz, dy) in enumerate(plane):
        dst = moved('z', dz) * size['y'] + moved('y', dy)
        sends.append(pltpu.make_async_remote_copy(
            src_ref=a_ref.at[dst], dst_ref=ar_ref.at[here], send_sem=a_send.at[j], recv_sem=a_recv.at[j],
            device_id={'z': moved('z', dz), 'y': moved('y', dy)}, device_id_type=mesh_id))
    for copy in sends:
        copy.start()
    ar_ref[here] = a_ref[here]
    for phase in range(1, 3):
        for part in range(2):
            for copy in flying[part]:
                copy.wait()
            flying[part] = spread(part, orders[part][phase], orders[part][:phase], phase * 2 + part)
    for part in range(2):
        for copy in flying[part]:
            copy.wait()
        flying[part] = spread(part, 'c', orders[part], 6 + part)
    for copy in sends:
        copy.wait()
    heads = out_ref.shape[0]
    per = bias_ref.shape[3] * bias_ref.shape[4] * bias_ref.shape[5]
    block = per // heads
    wide = bias_ref.shape[6]
    for part in range(2):
        for copy in flying[part]:
            copy.wait()

        def place(t, carry):
            x = bias_ref[part, t // size['y'], lax.rem(t, size['y'])].reshape(per, wide).astype(jnp.float32) * scale
            for kk in range(wide // LANES):
                tmp[kk] = x[:, kk * LANES:(kk + 1) * LANES]
            for kk in range(wide // LANES):
                for h in range(heads):
                    out_ref[h, pl.ds(pl.multiple_of(t * block, block), block), part * wide + kk * LANES:part * wide + (kk + 1) * LANES] = tmp[kk, pl.ds(h, block, stride=heads), :]
            return carry
        lax.fori_loop(0, size['z'] * size['y'], place, 0)


def exchange(rows, a_msg, sizes, heads, scale):
    half = rows.shape[1:]
    n = 2 * half[1]
    hops = max(sizes) - 1
    groups = sizes[0] * sizes[1]
    return pl.pallas_call(
        functools.partial(exchange_kernel, scale),
        out_shape=(jax.ShapeDtypeStruct((heads, n, n), jnp.float32), jax.ShapeDtypeStruct(a_msg.shape, jnp.bfloat16)),
        in_specs=[pl.BlockSpec(memory_space=pl.ANY), pl.BlockSpec(memory_space=pltpu.VMEM)],
        out_specs=(pl.BlockSpec(memory_space=pltpu.VMEM), pl.BlockSpec(memory_space=pltpu.VMEM)),
        scratch_shapes=[pltpu.VMEM((2,) + tuple(sizes) + half, jnp.bfloat16), pltpu.VMEM((half[1] // LANES, n // groups * heads, LANES), jnp.float32),
                        pltpu.SemaphoreType.DMA((2,)), pltpu.SemaphoreType.DMA((8, hops)), pltpu.SemaphoreType.DMA((8, hops)),
                        pltpu.SemaphoreType.DMA((groups - 1,)), pltpu.SemaphoreType.DMA((groups - 1,))],
        compiler_params=pltpu.CompilerParams(collective_id=0, has_side_effects=True, vmem_limit_bytes=VMEM_LIMIT),
        cost_estimate=pl.CostEstimate(flops=10_000_000_000, bytes_accessed=10_000_000, transcendentals=0),
        name="exchange",
    )(rows, a_msg)


def solution(mesh):
    devices = mesh.devices
    fine = Mesh(devices.reshape(devices.shape[0], 4, 4, 4, 2), ('data', 'z', 'y', 'x', 'c'))
    seq_spec = P(('data',) + ALL_AXES)

    def per_device(msa, msa_mask, pair_act, opm_gain, opm_shift, proj_a, bias_a, proj_b, bias_b, proj_out, bias_out, row_gain, row_shift, pair_gain, pair_proj, query_w, key_w, value_w, gate_w, gate_bias, attn_out_w, attn_out_b):
        seqs, n, cm = msa.shape
        rows_dev, _, ce = pair_act.shape
        ch = proj_a.shape[1]
        groups = fine.shape['z'] * fine.shape['y']
        rows = n // groups

        a_msg, b_loc = project_ab(msa, msa_mask, opm_gain, opm_shift, proj_a, bias_a, proj_b, bias_b)
        b_all = lax.all_gather(b_loc, GROUP_AXES, axis=0, tiled=False)

        pair_in, a_msg = lax.optimization_barrier((pair_act, a_msg))
        pair_c = pair_in - jnp.mean(pair_in, axis=-1, keepdims=True)
        pair_var = jnp.mean(jnp.square(pair_c), axis=-1, keepdims=True)
        pair_n = (pair_c * lax.rsqrt(pair_var + LN_EPS) * pair_gain.astype(jnp.float32)).astype(jnp.bfloat16)
        bias_rows = jnp.einsum('ije,eh->ihj', pair_n, pair_proj, preferred_element_type=jnp.float32).astype(jnp.bfloat16)
        heads = bias_rows.shape[1]
        bias_rows = bias_rows.reshape(rows_dev, heads, 2, n // 2).transpose(2, 0, 1, 3).reshape(2, rows_dev * heads, n // 2)
        sizes = tuple(fine.shape[ax] for ax in ALL_AXES)
        near, rest_scale = split_scale(cm // heads)
        pair_bias, a_recv = exchange(bias_rows, a_msg, sizes, heads, 1.0 / rest_scale)

        attend = functools.partial(attention, msa, msa_mask, pair_bias, row_gain, row_shift, query_w, key_w, value_w, gate_w, gate_bias, attn_out_w, attn_out_b)
        early = seqs // 2
        msa_new = attend(0, early)
        a_recv, msa_new = lax.optimization_barrier((a_recv, msa_new))

        p_t = proj_out.reshape(ch, ch, ce).transpose(1, 2, 0).reshape(ch * ce, ch)
        first = lax.axis_index(GROUP_AXES) * rows
        order = lax.broadcasted_iota(jnp.int32, (rows // 2, n), 0)
        cols = lax.broadcasted_iota(jnp.int32, (rows // 2, n), 1)
        totals = []
        for half in range(2):
            mine = first + (order // 2) * 4 + half * 2 + order % 2
            part = outer_product(a_recv, p_t, b_all, (cols == mine).astype(jnp.bfloat16), half)
            totals.append(lax.psum_scatter(part, SPLIT_AXES, scatter_dimension=0, tiled=True))
        msa_new, _ = lax.optimization_barrier((msa_new, part))
        msa_new = attend(early, seqs - early, msa_new)
        total = jnp.concatenate(totals, axis=0)
        outer_sum = total[:, :ce].transpose(0, 2, 1)
        counts = total[:, ce]
        pair_new = pair_act + (outer_sum + bias_out.astype(jnp.float32)) / (COUNT_EPS + counts)[:, :, None]
        return msa_new, pair_new

    in_specs = (seq_spec, seq_spec, seq_spec) + (P(),) * 19
    return jax.shard_map(per_device, mesh=fine, in_specs=in_specs, out_specs=(seq_spec, seq_spec), check_vma=False)
```

```python
import functools
import math
import jax
import jax.numpy as jnp
from jax import lax
from jax.experimental import pallas as pl
from jax.experimental.pallas import tpu as pltpu
from jax.sharding import Mesh, PartitionSpec as P

LN_EPS = 1e-5
COUNT_EPS = 1e-3
MASK_FILL = -1e9
LOG2E = math.log2(math.e)
VMEM_LIMIT = 60 * 1024 * 1024
LANES = 128
SUBLANES = 8
ALL_AXES = ('z', 'y', 'x', 'c')
GROUP_AXES = ('z', 'y')
SPLIT_AXES = ('x', 'c')


def attn_kernel(first, msa_ref, mask_ref, bias_ref, gain_ref, shift_ref, qw_ref, kw_ref, vw_ref, gw_ref, gb_ref, wo_ref, bo_ref, *rest):
    out_ref, q_scr, k_scr, v_scr, g_scr, w_scr, vb_scr = rest[-7:]
    n, cm = msa_ref.shape[1:]
    heads = bias_ref.shape[0]
    hd = cm // heads
    near, rest_scale = split_scale(hd)
    x = msa_ref[0].astype(jnp.float32)
    mu = jnp.mean(x, axis=-1, keepdims=True)
    xc = x - mu
    var = jnp.mean(xc * xc, axis=-1, keepdims=True)
    r = (xc * lax.rsqrt(var + LN_EPS) * gain_ref[...].astype(jnp.float32) + shift_ref[...].astype(jnp.float32)).astype(jnp.bfloat16)
    q_scr[...] = jnp.dot(r, qw_ref[...], preferred_element_type=jnp.float32).astype(jnp.bfloat16) * jnp.bfloat16(near)
    k_scr[...] = jnp.dot(r, kw_ref[...], preferred_element_type=jnp.float32).astype(jnp.bfloat16)
    v = jnp.dot(r, vw_ref[...], preferred_element_type=jnp.float32).astype(jnp.bfloat16)
    g_scr[...] = jax.nn.sigmoid(jnp.dot(r, gw_ref[...], preferred_element_type=jnp.float32) + gb_ref[...].astype(jnp.float32)).astype(jnp.bfloat16)
    lane_head = lax.broadcasted_iota(jnp.int32, (1, cm), 1) // hd
    for h in range(heads):
        vb_scr[h * n:(h + 1) * n, :] = v * (lane_head == h).astype(jnp.bfloat16)
    keep = mask_ref[pl.ds(pl.program_id(0) + first, 1), :] > 0
    q = q_scr[...]
    for h in range(heads):
        qh = q * (lane_head == h).astype(jnp.bfloat16)
        s = lax.dot_general(qh, k_scr[...], (((1,), (1,)), ((), ())), preferred_element_type=jnp.float32)
        s = jnp.where(keep, s + bias_ref[h], MASK_FILL / rest_scale)
        m = jnp.max(s, axis=-1, keepdims=True)
        e = jnp.exp2((s - m) * (rest_scale * LOG2E))
        l = jnp.sum(e, axis=-1, keepdims=True)
        w_scr[:, h * n:(h + 1) * n] = (e * (1.0 / l)).astype(jnp.bfloat16)
    o = jnp.dot(w_scr[...], vb_scr[...], preferred_element_type=jnp.float32)
    o = (o * g_scr[...].astype(jnp.float32)).astype(jnp.bfloat16)
    u = jnp.dot(o, wo_ref[...], preferred_element_type=jnp.float32) + bo_ref[...].astype(jnp.float32)
    out_ref[0] = (msa_ref[0].astype(jnp.float32) + u).astype(jnp.bfloat16)


def split_scale(hd):
    near = 2.0 ** math.floor(math.log2(hd ** -0.5))
    return near, hd ** -0.5 / near


def attention(msa, mask, bias, gain, shift, qw, kw, vw, gw, gb, wo, bo, first, count, before=None):
    s, n, cm = msa.shape
    heads = bias.shape[0]
    const = lambda shape: pl.BlockSpec(shape, lambda i: (0,) * len(shape), pipeline_mode=pl.Buffered(1))
    extra = () if before is None else (before,)
    return pl.pallas_call(
        functools.partial(attn_kernel, first),
        out_shape=jax.ShapeDtypeStruct((s, n, cm), jnp.bfloat16),
        grid=(count,),
        in_specs=[pl.BlockSpec((1, n, cm), lambda i: (i + first, 0, 0)), const((s, n)),
                  const((heads, n, n)), const((1, cm)), const((1, cm)), const((cm, cm)), const((cm, cm)), const((cm, cm)), const((cm, cm)), const((1, cm)), const((cm, cm)), const((1, cm))]
                 + [pl.BlockSpec(memory_space=pl.ANY)] * len(extra),
        out_specs=pl.BlockSpec((1, n, cm), lambda i: (i + first, 0, 0)),
        scratch_shapes=[pltpu.VMEM((n, cm), jnp.bfloat16)] * 4 + [pltpu.VMEM((n, heads * n), jnp.bfloat16), pltpu.VMEM((heads * n, cm), jnp.bfloat16)],
        input_output_aliases={12: 0} if extra else {},
        compiler_params=pltpu.CompilerParams(vmem_limit_bytes=VMEM_LIMIT, dimension_semantics=("arbitrary",)),
        cost_estimate=pl.CostEstimate(flops=count * 1_500_000_000, bytes_accessed=20_000_000, transcendentals=count * 2_000_000),
        name="row_attention",
    )(msa, mask, bias, gain[None], shift[None], qw, kw, vw, gw, gb[None], wo, bo[None], *extra)


def ab_kernel(msa_ref, mask_ref, gain_ref, shift_ref, pa_ref, ba_ref, pb_ref, bb_ref, a_ref, b_ref, scr_a, scr_b):
    seqs, n, cm = msa_ref.shape
    ch = scr_b.shape[0]
    quads = n // LANES
    subs = a_ref.shape[0] // quads
    width = LANES // subs
    lane = lax.broadcasted_iota(jnp.int32, (SUBLANES, LANES), 1) // width
    w = jnp.concatenate([pa_ref[...], pb_ref[...]], axis=1).astype(jnp.float32).T.astype(jnp.bfloat16)
    bias = jnp.concatenate([ba_ref[...], bb_ref[...]], axis=1).astype(jnp.float32)
    bias = jnp.broadcast_to(bias, (SUBLANES, 2 * ch)).T[:, 0:1]
    gain = gain_ref[...].astype(jnp.float32)
    shift = shift_ref[...].astype(jnp.float32)

    def one(s, carry):
        x = msa_ref[s].astype(jnp.float32)
        mu = jnp.mean(x, axis=-1, keepdims=True)
        xc = x - mu
        var = jnp.mean(xc * xc, axis=-1, keepdims=True)
        xn = (xc * lax.rsqrt(var + LN_EPS) * gain + shift).astype(jnp.bfloat16)
        y = lax.dot_general(w, xn, (((1,), (1,)), ((), ())), preferred_element_type=jnp.float32)
        y = (y + bias) * mask_ref[pl.ds(s, 1), :].astype(jnp.float32)
        scr_b[:, pl.ds(s, 1), :] = y[ch:2 * ch].reshape(ch, 1, n)
        for zz in range(quads):
            tiles = [y[c4 * SUBLANES:(c4 + 1) * SUBLANES, zz * LANES:(zz + 1) * LANES] for c4 in range(subs)]
            for yy in range(subs):
                out = tiles[yy]
                for c4 in range(subs):
                    if c4 != yy:
                        out = jnp.where(lane == c4, pltpu.roll(tiles[c4], ((c4 - yy) * width) % LANES, 1), out)
                scr_a[zz * subs + yy, pl.ds(pl.multiple_of(s * SUBLANES, SUBLANES), SUBLANES), :] = out
        return carry
    lax.fori_loop(0, seqs, one, 0)
    a_ref[...] = scr_a[...].astype(jnp.bfloat16)
    b_ref[0:ch] = scr_b[...].astype(jnp.bfloat16)
    b_ref[ch] = mask_ref[...].astype(jnp.float32).astype(jnp.bfloat16)


def project_ab(msa, mask, gain, shift, proj_a, bias_a, proj_b, bias_b):
    s, n, cm = msa.shape
    ch = proj_a.shape[1]
    return pl.pallas_call(
        ab_kernel,
        out_shape=(jax.ShapeDtypeStruct((16, s * SUBLANES, LANES), jnp.bfloat16), jax.ShapeDtypeStruct((ch + 1, s, n), jnp.bfloat16)),
        scratch_shapes=[pltpu.VMEM((16, s * SUBLANES, LANES), jnp.float32), pltpu.VMEM((ch, s, n), jnp.float32)],
        compiler_params=pltpu.CompilerParams(vmem_limit_bytes=VMEM_LIMIT),
        cost_estimate=pl.CostEstimate(flops=300_000_000, bytes_accessed=6_000_000, transcendentals=8192),
        name="project_ab",
    )(msa, mask, gain[None], shift[None], proj_a, bias_a[None], proj_b, bias_b[None])


def opm_kernel(db, ib, u_ref, b_ref, m_ref, sel_ref, out_ref):
    rows, wide, n = out_ref.shape
    ce = u_ref.shape[0] // rows
    k = m_ref.shape[0] * m_ref.shape[2]

    @pl.when(pl.program_id(0) == 0)
    def _():
        m = m_ref[...].reshape(k, n)
        mi = lax.dot_general(sel_ref[...], m, (((1,), (1,)), ((), ())), preferred_element_type=jnp.float32).astype(jnp.bfloat16)
        cnt = jnp.dot(mi, m, preferred_element_type=jnp.float32)
        for i in range(rows):
            out_ref[i, 0:ce, :] = jnp.zeros((ce, n), jnp.float32)
            out_ref[i, ce:, :] = jnp.broadcast_to(cnt[i:i + 1, :], (wide - ce, n))

    bk = jnp.concatenate([b_ref[:, dd].reshape(k, n) for dd in range(db)], axis=0)

    def block(g, carry):
        size = ib * ce
        part = jnp.dot(u_ref[pl.ds(pl.multiple_of(g * size, size), size), :], bk, preferred_element_type=jnp.float32)
        for ii in range(ib):
            out_ref[g * ib + ii, 0:ce, :] += part[ii * ce:(ii + 1) * ce]
        return carry
    lax.fori_loop(0, rows // ib, block, 0)


def outer_product(u, b_all, sel, half, db=4, ib=8):
    rows, n = sel.shape
    src, ch, s, _ = b_all.shape
    ch -= 1
    ce = u.shape[0] // (2 * rows)
    k = src * s
    return pl.pallas_call(
        functools.partial(opm_kernel, db, ib),
        out_shape=jax.ShapeDtypeStruct((rows, ce + SUBLANES, n), jnp.float32),
        grid=(ch // db,),
        in_specs=[pl.BlockSpec((rows * ce, db * k), lambda g: (half, g)),
                  pl.BlockSpec((src, db, s, n), lambda g: (0, g, 0, 0)),
                  pl.BlockSpec((src, 1, s, n), lambda g: (0, ch, 0, 0)),
                  pl.BlockSpec((rows, n), lambda g: (0, 0))],
        out_specs=pl.BlockSpec((rows, ce + SUBLANES, n), lambda g: (0, 0, 0)),
        compiler_params=pltpu.CompilerParams(vmem_limit_bytes=VMEM_LIMIT, dimension_semantics=("arbitrary",)),
        cost_estimate=pl.CostEstimate(flops=2 * rows * ce * n * k * ch, bytes_accessed=50_000_000, transcendentals=0),
        name="outer_product",
    )(u, b_all, b_all, sel)


def turn_a(ar_ref, at_ref, af, at2):
    k = af.shape[0] // SUBLANES
    rows, ch = 2 * at_ref.shape[0], at_ref.shape[1]
    af[...] = ar_ref[...].reshape(af.shape).astype(jnp.float32)
    eye = (lax.broadcasted_iota(jnp.int32, (LANES, LANES), 0) == lax.broadcasted_iota(jnp.int32, (LANES, LANES), 1)).astype(jnp.bfloat16)
    for c8 in range(SUBLANES):
        x = af[pl.ds(c8, k, stride=SUBLANES), :].astype(jnp.bfloat16)
        t = lax.dot_general(eye, x, (((1,), (1,)), ((), ())), preferred_element_type=jnp.float32)
        for c4 in range(ch // SUBLANES):
            for kk in range(k // LANES):
                at2[kk, pl.ds(c4 * SUBLANES + c8, rows, stride=ch), :] = t[c4 * rows:(c4 + 1) * rows, kk * LANES:(kk + 1) * LANES]
    for par in range(2):
        for kk in range(k // LANES):
            both = at2[kk].reshape(rows // 2, 2 * ch, LANES)[:, par * ch:(par + 1) * ch]
            at_ref[:, :, par * k + kk * LANES:par * k + (kk + 1) * LANES] = both.astype(jnp.bfloat16)


def u_rows(t, at_ref, pt_ref, slab, u_ref, sem, ce, per):
    pairs, ch, k = at_ref.shape
    k //= 2
    slot = lax.rem(t, 2)
    row = slot * pairs + (t // 2) * 2
    copy = pltpu.make_async_copy(slab.at[slot], u_ref.at[pl.ds(pl.multiple_of(row * ce, 2 * ce), 2 * ce), :], sem.at[slot])

    @pl.when(t >= 2)
    def _():
        copy.wait()

    def some(p, carry):
        u = jnp.dot(pt_ref[pl.ds(pl.multiple_of(p * per * ce, per * ce), per * ce), :], at_ref[t], preferred_element_type=jnp.float32).astype(jnp.bfloat16)
        for dd in range(per):
            for par in range(2):
                slab[slot, par * ce:(par + 1) * ce, pl.ds(pl.multiple_of((p * per + dd) * k, k), k)] = u[dd * ce:(dd + 1) * ce, par * k:(par + 1) * k]
        return carry
    lax.fori_loop(0, ch // per, some, 0)
    copy.start()


def exchange_kernel(scale, rows_ref, a_ref, pt_ref, out_ref, u_ref, ar_ref, bias_ref, tmp, at_ref, af, at2, slab, slab_sem, own_sem, send_sem, recv_sem, a_send, a_recv):
    mesh_id = pl.DeviceIdType.MESH
    me = {name: lax.axis_index(name) for name in ALL_AXES}
    size = {'z': bias_ref.shape[1], 'y': bias_ref.shape[2], 'x': bias_ref.shape[3], 'c': bias_ref.shape[4]}

    def moved(name, k):
        return lax.rem(me[name] + k, size[name])

    plane = [(dz, dy) for dz in range(size['z']) for dy in range(size['y']) if dz or dy]
    barrier = pltpu.get_barrier_semaphore()
    peers = [{'z': moved('z', dz), 'y': moved('y', dy)} for dz, dy in plane]
    peers += [{'x': moved('x', k)} for k in range(1, size['x'])] + [{'c': moved('c', k)} for k in range(1, size['c'])]
    for peer in peers:
        pl.semaphore_signal(barrier, inc=1, device_id=peer, device_id_type=mesh_id)

    own = [pltpu.make_async_copy(rows_ref.at[part], bias_ref.at[part, me['z'], me['y'], me['x'], me['c']], own_sem.at[part]) for part in range(2)]
    for copy in own:
        copy.start()
    pl.semaphore_wait(barrier, len(peers))

    def spread(part, name, done, slot):
        where = tuple(pl.ds(0, size[ax]) if ax in done else me[ax] for ax in ALL_AXES)
        ref = bias_ref.at[(part,) + where]
        copies = []
        for k in range(1, size[name]):
            copies.append(pltpu.make_async_remote_copy(
                src_ref=ref, dst_ref=ref, send_sem=send_sem.at[slot, k - 1], recv_sem=recv_sem.at[slot, k - 1],
                device_id={name: moved(name, k)}, device_id_type=mesh_id))
        for copy in copies:
            copy.start()
        return copies

    for copy in own:
        copy.wait()
    orders = (('x', 'y', 'z'), ('z', 'x', 'y'))
    flying = [spread(part, orders[part][0], (), part) for part in range(2)]
    here = me['z'] * size['y'] + me['y']
    sends = []
    for j, (dz, dy) in enumerate(plane):
        dst = moved('z', dz) * size['y'] + moved('y', dy)
        sends.append(pltpu.make_async_remote_copy(
            src_ref=a_ref.at[dst], dst_ref=ar_ref.at[here], send_sem=a_send.at[j], recv_sem=a_recv.at[j],
            device_id={'z': moved('z', dz), 'y': moved('y', dy)}, device_id_type=mesh_id))
    for copy in sends:
        copy.start()
    ar_ref[here] = a_ref[here]

    def advance(phase):
        for part in range(2):
            for copy in flying[part]:
                copy.wait()
            if phase < 3:
                flying[part] = spread(part, orders[part][phase], orders[part][:phase], phase * 2 + part)
            else:
                flying[part] = spread(part, 'c', orders[part], 6 + part)

    pairs = at_ref.shape[0]
    ce = slab.shape[1] // 2

    def run(lo, hi):
        def body(t, carry):
            u_rows(t, at_ref, pt_ref, slab, u_ref, slab_sem, ce, 16)
            return carry
        lax.fori_loop(lo, hi, body, 0)

    advance(1)
    for copy in sends:
        copy.wait()
    turn_a(ar_ref, at_ref, af, at2)
    run(0, pairs // 4)
    advance(2)
    run(pairs // 4, 3 * pairs // 4)
    advance(3)
    run(3 * pairs // 4, pairs)
    heads = out_ref.shape[0]
    per = bias_ref.shape[3] * bias_ref.shape[4] * bias_ref.shape[5]
    block = per // heads
    wide = bias_ref.shape[6]
    for part in range(2):
        for copy in flying[part]:
            copy.wait()

        def place(t, carry):
            x = bias_ref[part, t // size['y'], lax.rem(t, size['y'])].reshape(per, wide).astype(jnp.float32) * scale
            for kk in range(wide // LANES):
                tmp[kk] = x[:, kk * LANES:(kk + 1) * LANES]
            for kk in range(wide // LANES):
                for h in range(heads):
                    out_ref[h, pl.ds(pl.multiple_of(t * block, block), block), part * wide + kk * LANES:part * wide + (kk + 1) * LANES] = tmp[kk, pl.ds(h, block, stride=heads), :]
            return carry
        lax.fori_loop(0, size['z'] * size['y'], place, 0)
    for s in range(2):
        pltpu.make_async_copy(slab.at[s], u_ref.at[pl.ds(0, 2 * ce), :], slab_sem.at[s]).wait()


def exchange(rows, a_msg, p_t, sizes, heads, scale):
    half = rows.shape[1:]
    n = 2 * half[1]
    hops = max(sizes) - 1
    groups = sizes[0] * sizes[1]
    ch = p_t.shape[1]
    ce = p_t.shape[0] // ch
    mine = n // groups
    k = a_msg.shape[0] * a_msg.shape[1] // SUBLANES
    return pl.pallas_call(
        functools.partial(exchange_kernel, scale),
        out_shape=(jax.ShapeDtypeStruct((heads, n, n), jnp.float32), jax.ShapeDtypeStruct((mine * ce, ch * k), jnp.bfloat16)),
        in_specs=[pl.BlockSpec(memory_space=pl.ANY), pl.BlockSpec(memory_space=pltpu.VMEM), pl.BlockSpec(memory_space=pltpu.VMEM)],
        out_specs=(pl.BlockSpec(memory_space=pltpu.VMEM), pl.BlockSpec(memory_space=pl.ANY)),
        scratch_shapes=[pltpu.VMEM(a_msg.shape, jnp.bfloat16), pltpu.VMEM((2,) + tuple(sizes) + half, jnp.bfloat16), pltpu.VMEM((half[1] // LANES, n // groups * heads, LANES), jnp.float32),
                        pltpu.VMEM((mine // 2, ch, 2 * k), jnp.bfloat16), pltpu.VMEM((k * SUBLANES, LANES), jnp.float32), pltpu.VMEM((k // LANES, mine * ch, LANES), jnp.float32),
                        pltpu.VMEM((2, 2 * ce, ch * k), jnp.bfloat16), pltpu.SemaphoreType.DMA((2,)),
                        pltpu.SemaphoreType.DMA((2,)), pltpu.SemaphoreType.DMA((8, hops)), pltpu.SemaphoreType.DMA((8, hops)),
                        pltpu.SemaphoreType.DMA((groups - 1,)), pltpu.SemaphoreType.DMA((groups - 1,))],
        compiler_params=pltpu.CompilerParams(collective_id=0, has_side_effects=True, vmem_limit_bytes=VMEM_LIMIT),
        cost_estimate=pl.CostEstimate(flops=10_000_000_000, bytes_accessed=10_000_000, transcendentals=0),
        name="exchange",
    )(rows, a_msg, p_t)


def solution(mesh):
    devices = mesh.devices
    fine = Mesh(devices.reshape(devices.shape[0], 4, 4, 4, 2), ('data', 'z', 'y', 'x', 'c'))
    seq_spec = P(('data',) + ALL_AXES)

    def per_device(msa, msa_mask, pair_act, opm_gain, opm_shift, proj_a, bias_a, proj_b, bias_b, proj_out, bias_out, row_gain, row_shift, pair_gain, pair_proj, query_w, key_w, value_w, gate_w, gate_bias, attn_out_w, attn_out_b):
        seqs, n, cm = msa.shape
        rows_dev, _, ce = pair_act.shape
        ch = proj_a.shape[1]
        groups = fine.shape['z'] * fine.shape['y']
        rows = n // groups

        a_msg, b_loc = project_ab(msa, msa_mask, opm_gain, opm_shift, proj_a, bias_a, proj_b, bias_b)
        b_all = lax.all_gather(b_loc, GROUP_AXES, axis=0, tiled=False)

        pair_in, a_msg = lax.optimization_barrier((pair_act, a_msg))
        pair_c = pair_in - jnp.mean(pair_in, axis=-1, keepdims=True)
        pair_var = jnp.mean(jnp.square(pair_c), axis=-1, keepdims=True)
        pair_n = (pair_c * lax.rsqrt(pair_var + LN_EPS) * pair_gain.astype(jnp.float32)).astype(jnp.bfloat16)
        bias_rows = jnp.einsum('ije,eh->ihj', pair_n, pair_proj, preferred_element_type=jnp.float32).astype(jnp.bfloat16)
        heads = bias_rows.shape[1]
        bias_rows = bias_rows.reshape(rows_dev, heads, 2, n // 2).transpose(2, 0, 1, 3).reshape(2, rows_dev * heads, n // 2)
        sizes = tuple(fine.shape[ax] for ax in ALL_AXES)
        near, rest_scale = split_scale(cm // heads)
        p_t = proj_out.reshape(ch, ch, ce).transpose(1, 2, 0).reshape(ch * ce, ch)
        pair_bias, u = exchange(bias_rows, a_msg, p_t, sizes, heads, 1.0 / rest_scale)

        attend = functools.partial(attention, msa, msa_mask, pair_bias, row_gain, row_shift, query_w, key_w, value_w, gate_w, gate_bias, attn_out_w, attn_out_b)
        early = seqs * 7 // 16
        msa_new = attend(0, early)

        first = lax.axis_index(GROUP_AXES) * rows
        order = lax.broadcasted_iota(jnp.int32, (rows // 2, n), 0)
        cols = lax.broadcasted_iota(jnp.int32, (rows // 2, n), 1)
        picks = [(cols == first + (order // 2) * 4 + half * 2 + order % 2).astype(jnp.bfloat16) for half in range(2)]
        picks, msa_new = lax.optimization_barrier((picks, msa_new))
        totals = []
        for half in range(2):
            part = outer_product(u, b_all, picks[half], half, ib=16)
            totals.append(lax.psum_scatter(part, SPLIT_AXES, scatter_dimension=0, tiled=True))
        msa_new, _ = lax.optimization_barrier((msa_new, part))
        msa_new = attend(early, seqs - early, msa_new)
        total = jnp.concatenate(totals, axis=0)
        outer_sum = total[:, :ce].transpose(0, 2, 1)
        counts = total[:, ce]
        pair_new = pair_act + (outer_sum + bias_out.astype(jnp.float32)) / (COUNT_EPS + counts)[:, :, None]
        return msa_new, pair_new

    in_specs = (seq_spec, seq_spec, seq_spec) + (P(),) * 19
    return jax.shard_map(per_device, mesh=fine, in_specs=in_specs, out_specs=(seq_spec, seq_spec), check_vma=False)
```

```python
import functools
import math
import jax
import jax.numpy as jnp
from jax import lax
from jax.experimental import pallas as pl
from jax.experimental.pallas import tpu as pltpu
from jax.sharding import Mesh, PartitionSpec as P

LN_EPS = 1e-5
COUNT_EPS = 1e-3
MASK_FILL = -1e9
LOG2E = math.log2(math.e)
VMEM_LIMIT = 60 * 1024 * 1024
LANES = 128
SUBLANES = 8
ALL_AXES = ('z', 'y', 'x', 'c')
GROUP_AXES = ('z', 'y')
SPLIT_AXES = ('x', 'c')


def attn_kernel(first, msa_ref, mask_ref, bias_ref, gain_ref, shift_ref, qw_ref, kw_ref, vw_ref, gw_ref, gb_ref, wo_ref, bo_ref, *rest):
    out_ref, q_scr, k_scr, v_scr, g_scr, w_scr, vb_scr = rest[-7:]
    n, cm = msa_ref.shape[1:]
    heads = bias_ref.shape[0]
    hd = cm // heads
    near, rest_scale = split_scale(hd)
    x = msa_ref[0].astype(jnp.float32)
    mu = jnp.mean(x, axis=-1, keepdims=True)
    xc = x - mu
    var = jnp.mean(xc * xc, axis=-1, keepdims=True)
    r = (xc * lax.rsqrt(var + LN_EPS) * gain_ref[...].astype(jnp.float32).reshape(1, cm) + shift_ref[...].astype(jnp.float32).reshape(1, cm)).astype(jnp.bfloat16)
    q_scr[...] = jnp.dot(r, qw_ref[...], preferred_element_type=jnp.float32).astype(jnp.bfloat16) * jnp.bfloat16(near)
    k_scr[...] = jnp.dot(r, kw_ref[...], preferred_element_type=jnp.float32).astype(jnp.bfloat16)
    v = jnp.dot(r, vw_ref[...], preferred_element_type=jnp.float32).astype(jnp.bfloat16)
    g_scr[...] = jax.nn.sigmoid(jnp.dot(r, gw_ref[...], preferred_element_type=jnp.float32) + gb_ref[...].astype(jnp.float32).reshape(1, cm)).astype(jnp.bfloat16)
    lane_head = lax.broadcasted_iota(jnp.int32, (1, cm), 1) // hd
    for h in range(heads):
        vb_scr[h * n:(h + 1) * n, :] = v * (lane_head == h).astype(jnp.bfloat16)
    keep = mask_ref[pl.ds(pl.program_id(0) + first, 1), :] > 0
    q = q_scr[...]
    for h in range(heads):
        qh = q * (lane_head == h).astype(jnp.bfloat16)
        s = lax.dot_general(qh, k_scr[...], (((1,), (1,)), ((), ())), preferred_element_type=jnp.float32)
        s = jnp.where(keep, s + bias_ref[h], MASK_FILL / rest_scale)
        m = jnp.max(s, axis=-1, keepdims=True)
        e = jnp.exp2((s - m) * (rest_scale * LOG2E))
        l = jnp.sum(e, axis=-1, keepdims=True)
        w_scr[:, h * n:(h + 1) * n] = (e * (1.0 / l)).astype(jnp.bfloat16)
    o = jnp.dot(w_scr[...], vb_scr[...], preferred_element_type=jnp.float32)
    o = (o * g_scr[...].astype(jnp.float32)).astype(jnp.bfloat16)
    u = jnp.dot(o, wo_ref[...], preferred_element_type=jnp.float32) + bo_ref[...].astype(jnp.float32).reshape(1, cm)
    out_ref[0] = (msa_ref[0].astype(jnp.float32) + u).astype(jnp.bfloat16)


def split_scale(hd):
    near = 2.0 ** math.floor(math.log2(hd ** -0.5))
    return near, hd ** -0.5 / near


def attention(msa, mask, bias, gain, shift, qw, kw, vw, gw, gb, wo, bo, first, count, before=None):
    s, n, cm = msa.shape
    heads = bias.shape[0]
    const = lambda shape: pl.BlockSpec(shape, lambda i: (0,) * len(shape), pipeline_mode=pl.Buffered(1))
    extra = () if before is None else (before,)
    return pl.pallas_call(
        functools.partial(attn_kernel, first),
        out_shape=jax.ShapeDtypeStruct((s, n, cm), jnp.bfloat16),
        grid=(count,),
        in_specs=[pl.BlockSpec((1, n, cm), lambda i: (i + first, 0, 0)), const((s, n)),
                  const((heads, n, n)), const((cm,)), const((cm,)), const((cm, cm)), const((cm, cm)), const((cm, cm)), const((cm, cm)), const((cm,)), const((cm, cm)), const((cm,))]
                 + [pl.BlockSpec(memory_space=pl.ANY)] * len(extra),
        out_specs=pl.BlockSpec((1, n, cm), lambda i: (i + first, 0, 0)),
        scratch_shapes=[pltpu.VMEM((n, cm), jnp.bfloat16)] * 4 + [pltpu.VMEM((n, heads * n), jnp.bfloat16), pltpu.VMEM((heads * n, cm), jnp.bfloat16)],
        input_output_aliases={12: 0} if extra else {},
        compiler_params=pltpu.CompilerParams(vmem_limit_bytes=VMEM_LIMIT, dimension_semantics=("arbitrary",)),
        cost_estimate=pl.CostEstimate(flops=count * 1_500_000_000, bytes_accessed=20_000_000, transcendentals=count * 2_000_000),
        name="row_attention",
    )(msa, mask, bias, gain, shift, qw, kw, vw, gw, gb, wo, bo, *extra)


def ab_kernel(msa_ref, mask_ref, gain_ref, shift_ref, pa_ref, ba_ref, pb_ref, bb_ref, a_ref, b_ref, scr_a, scr_b):
    seqs, n, cm = msa_ref.shape
    ch = scr_b.shape[0]
    quads = n // LANES
    subs = a_ref.shape[0] // quads
    width = LANES // subs
    lane = lax.broadcasted_iota(jnp.int32, (SUBLANES, LANES), 1) // width
    w = jnp.concatenate([pa_ref[...], pb_ref[...]], axis=0)
    bias = jnp.concatenate([ba_ref[...].astype(jnp.float32).reshape(1, ch), bb_ref[...].astype(jnp.float32).reshape(1, ch)], axis=1)
    bias = jnp.broadcast_to(bias, (SUBLANES, 2 * ch)).T[:, 0:1]
    gain = gain_ref[...].astype(jnp.float32).reshape(1, cm)
    shift = shift_ref[...].astype(jnp.float32).reshape(1, cm)

    def one(s, carry):
        x = msa_ref[s].astype(jnp.float32)
        mu = jnp.mean(x, axis=-1, keepdims=True)
        xc = x - mu
        var = jnp.mean(xc * xc, axis=-1, keepdims=True)
        xn = (xc * lax.rsqrt(var + LN_EPS) * gain + shift).astype(jnp.bfloat16)
        y = lax.dot_general(w, xn, (((1,), (1,)), ((), ())), preferred_element_type=jnp.float32)
        y = (y + bias) * mask_ref[pl.ds(s, 1), :].astype(jnp.float32)
        scr_b[:, pl.ds(s, 1), :] = y[ch:2 * ch].reshape(ch, 1, n)
        for zz in range(quads):
            tiles = [y[c4 * SUBLANES:(c4 + 1) * SUBLANES, zz * LANES:(zz + 1) * LANES] for c4 in range(subs)]
            for yy in range(subs):
                out = tiles[yy]
                for c4 in range(subs):
                    if c4 != yy:
                        out = jnp.where(lane == c4, pltpu.roll(tiles[c4], ((c4 - yy) * width) % LANES, 1), out)
                scr_a[zz * subs + yy, pl.ds(pl.multiple_of(s * SUBLANES, SUBLANES), SUBLANES), :] = out
        return carry
    lax.fori_loop(0, seqs, one, 0, unroll=2)
    a_ref[...] = scr_a[...].astype(jnp.bfloat16)
    b_ref[0:ch] = scr_b[...].astype(jnp.bfloat16)
    b_ref[ch] = mask_ref[...].astype(jnp.float32).astype(jnp.bfloat16)


def project_ab(msa, mask, gain, shift, proj_a, bias_a, proj_b, bias_b):
    s, n, cm = msa.shape
    ch = proj_a.shape[1]
    return pl.pallas_call(
        ab_kernel,
        out_shape=(jax.ShapeDtypeStruct((16, s * SUBLANES, LANES), jnp.bfloat16), jax.ShapeDtypeStruct((ch + 1, s, n), jnp.bfloat16)),
        scratch_shapes=[pltpu.VMEM((16, s * SUBLANES, LANES), jnp.float32), pltpu.VMEM((ch, s, n), jnp.float32)],
        compiler_params=pltpu.CompilerParams(vmem_limit_bytes=VMEM_LIMIT),
        cost_estimate=pl.CostEstimate(flops=300_000_000, bytes_accessed=6_000_000, transcendentals=8192),
        name="project_ab",
    )(msa, mask, gain, shift, proj_a.T, bias_a, proj_b.T, bias_b)


def opm_kernel(db, ib, u_ref, b_ref, m_ref, sel_ref, out_ref):
    rows, wide, n = out_ref.shape
    ce = u_ref.shape[0] // rows
    k = m_ref.shape[0] * m_ref.shape[2]

    @pl.when(pl.program_id(0) == 0)
    def _():
        m = m_ref[...].reshape(k, n)
        mi = lax.dot_general(sel_ref[...], m, (((1,), (1,)), ((), ())), preferred_element_type=jnp.float32).astype(jnp.bfloat16)
        cnt = jnp.dot(mi, m, preferred_element_type=jnp.float32)
        for i in range(rows):
            out_ref[i, 0:ce, :] = jnp.zeros((ce, n), jnp.float32)
            out_ref[i, ce:, :] = jnp.broadcast_to(cnt[i:i + 1, :], (wide - ce, n))

    bk = jnp.concatenate([b_ref[:, dd].reshape(k, n) for dd in range(db)], axis=0)

    def block(g, carry):
        size = ib * ce
        part = jnp.dot(u_ref[pl.ds(pl.multiple_of(g * size, size), size), :], bk, preferred_element_type=jnp.float32)
        for ii in range(ib):
            out_ref[g * ib + ii, 0:ce, :] += part[ii * ce:(ii + 1) * ce]
        return carry
    lax.fori_loop(0, rows // ib, block, 0)


def outer_product(u, b_all, sel, half, db=4, ib=8):
    rows, n = sel.shape
    src, ch, s, _ = b_all.shape
    ch -= 1
    ce = u.shape[0] // (2 * rows)
    k = src * s
    return pl.pallas_call(
        functools.partial(opm_kernel, db, ib),
        out_shape=jax.ShapeDtypeStruct((rows, ce + SUBLANES, n), jnp.float32),
        grid=(ch // db,),
        in_specs=[pl.BlockSpec((rows * ce, db * k), lambda g: (half, g)),
                  pl.BlockSpec((src, db, s, n), lambda g: (0, g, 0, 0)),
                  pl.BlockSpec((src, 1, s, n), lambda g: (0, ch, 0, 0)),
                  pl.BlockSpec((rows, n), lambda g: (0, 0))],
        out_specs=pl.BlockSpec((rows, ce + SUBLANES, n), lambda g: (0, 0, 0)),
        compiler_params=pltpu.CompilerParams(vmem_limit_bytes=VMEM_LIMIT, dimension_semantics=("arbitrary",)),
        cost_estimate=pl.CostEstimate(flops=2 * rows * ce * n * k * ch, bytes_accessed=50_000_000, transcendentals=0),
        name="outer_product",
    )(u, b_all, b_all, sel)


def turn_a(ar_ref, at_ref, af, at2):
    k = af.shape[0] // SUBLANES
    rows, ch = 2 * at_ref.shape[0], at_ref.shape[1]
    af[...] = ar_ref[...].reshape(af.shape).astype(jnp.float32)
    eye = (lax.broadcasted_iota(jnp.int32, (LANES, LANES), 0) == lax.broadcasted_iota(jnp.int32, (LANES, LANES), 1)).astype(jnp.bfloat16)
    for c8 in range(SUBLANES):
        x = af[pl.ds(c8, k, stride=SUBLANES), :].astype(jnp.bfloat16)
        t = lax.dot_general(eye, x, (((1,), (1,)), ((), ())), preferred_element_type=jnp.float32)
        for c4 in range(ch // SUBLANES):
            for kk in range(k // LANES):
                at2[kk, pl.ds(c4 * SUBLANES + c8, rows, stride=ch), :] = t[c4 * rows:(c4 + 1) * rows, kk * LANES:(kk + 1) * LANES]
    for par in range(2):
        for kk in range(k // LANES):
            both = at2[kk].reshape(rows // 2, 2 * ch, LANES)[:, par * ch:(par + 1) * ch]
            at_ref[:, :, par * k + kk * LANES:par * k + (kk + 1) * LANES] = both.astype(jnp.bfloat16)


def u_rows(t, at_ref, pt_ref, slab, u_ref, sem, ce, per):
    pairs, ch, k = at_ref.shape
    k //= 2
    slot = lax.rem(t, 2)
    row = slot * pairs + (t // 2) * 2
    copy = pltpu.make_async_copy(slab.at[slot], u_ref.at[pl.ds(pl.multiple_of(row * ce, 2 * ce), 2 * ce), :], sem.at[slot])

    @pl.when(t >= 2)
    def _():
        copy.wait()

    def some(p, carry):
        u = jnp.dot(pt_ref[pl.ds(pl.multiple_of(p * per * ce, per * ce), per * ce), :], at_ref[t], preferred_element_type=jnp.float32).astype(jnp.bfloat16)
        for dd in range(per):
            for par in range(2):
                slab[slot, par * ce:(par + 1) * ce, pl.ds(pl.multiple_of((p * per + dd) * k, k), k)] = u[dd * ce:(dd + 1) * ce, par * k:(par + 1) * k]
        return carry
    lax.fori_loop(0, ch // per, some, 0)
    copy.start()


def exchange_kernel(scale, rows_ref, a_ref, pt_ref, out_ref, u_ref, ar_ref, bias_ref, tmp, at_ref, af, at2, slab, slab_sem, own_sem, send_sem, recv_sem, a_send, a_recv):
    mesh_id = pl.DeviceIdType.MESH
    me = {name: lax.axis_index(name) for name in ALL_AXES}
    size = {'z': bias_ref.shape[1], 'y': bias_ref.shape[2], 'x': bias_ref.shape[3], 'c': bias_ref.shape[4]}

    def moved(name, k):
        return lax.rem(me[name] + k, size[name])

    plane = [(dz, dy) for dz in range(size['z']) for dy in range(size['y']) if dz or dy]
    barrier = pltpu.get_barrier_semaphore()
    peers = [{'z': moved('z', dz), 'y': moved('y', dy)} for dz, dy in plane]
    peers += [{'x': moved('x', k)} for k in range(1, size['x'])] + [{'c': moved('c', k)} for k in range(1, size['c'])]
    for peer in peers:
        pl.semaphore_signal(barrier, inc=1, device_id=peer, device_id_type=mesh_id)

    own = [pltpu.make_async_copy(rows_ref.at[part], bias_ref.at[part, me['z'], me['y'], me['x'], me['c']], own_sem.at[part]) for part in range(2)]
    for copy in own:
        copy.start()
    pl.semaphore_wait(barrier, len(peers))

    def spread(part, name, done, slot):
        where = tuple(pl.ds(0, size[ax]) if ax in done else me[ax] for ax in ALL_AXES)
        ref = bias_ref.at[(part,) + where]
        copies = []
        for k in range(1, size[name]):
            copies.append(pltpu.make_async_remote_copy(
                src_ref=ref, dst_ref=ref, send_sem=send_sem.at[slot, k - 1], recv_sem=recv_sem.at[slot, k - 1],
                device_id={name: moved(name, k)}, device_id_type=mesh_id))
        for copy in copies:
            copy.start()
        return copies

    orders = (('x', 'y', 'z'), ('z', 'x', 'y'))
    here = me['z'] * size['y'] + me['y']
    sends = []
    for j, (dz, dy) in enumerate(plane):
        dst = moved('z', dz) * size['y'] + moved('y', dy)
        sends.append(pltpu.make_async_remote_copy(
            src_ref=a_ref.at[dst], dst_ref=ar_ref.at[here], send_sem=a_send.at[j], recv_sem=a_recv.at[j],
            device_id={'z': moved('z', dz), 'y': moved('y', dy)}, device_id_type=mesh_id))
    for copy in sends:
        copy.start()
    ar_ref[here] = a_ref[here]
    for copy in own:
        copy.wait()
    flying = [spread(part, orders[part][0], (), part) for part in range(2)]

    def advance(phase):
        for part in range(2):
            for copy in flying[part]:
                copy.wait()
            if phase < 3:
                flying[part] = spread(part, orders[part][phase], orders[part][:phase], phase * 2 + part)
            else:
                flying[part] = spread(part, 'c', orders[part], 6 + part)

    pairs = at_ref.shape[0]
    ce = slab.shape[1] // 2

    def run(lo, hi):
        def body(t, carry):
            u_rows(t, at_ref, pt_ref, slab, u_ref, slab_sem, ce, 16)
            return carry
        lax.fori_loop(lo, hi, body, 0)

    for copy in sends:
        copy.wait()
    advance(1)
    turn_a(ar_ref, at_ref, af, at2)
    run(0, pairs // 4)
    advance(2)
    run(pairs // 4, 3 * pairs // 4)
    advance(3)
    run(3 * pairs // 4, pairs)
    heads = out_ref.shape[0]
    per = bias_ref.shape[3] * bias_ref.shape[4] * bias_ref.shape[5]
    block = per // heads
    wide = bias_ref.shape[6]
    for part in range(2):
        for copy in flying[part]:
            copy.wait()

        def place(t, carry):
            x = bias_ref[part, t // size['y'], lax.rem(t, size['y'])].reshape(per, wide).astype(jnp.float32) * scale
            for kk in range(wide // LANES):
                tmp[kk] = x[:, kk * LANES:(kk + 1) * LANES]
            for kk in range(wide // LANES):
                for h in range(heads):
                    out_ref[h, pl.ds(pl.multiple_of(t * block, block), block), part * wide + kk * LANES:part * wide + (kk + 1) * LANES] = tmp[kk, pl.ds(h, block, stride=heads), :]
            return carry
        lax.fori_loop(0, size['z'] * size['y'], place, 0)
    for s in range(2):
        pltpu.make_async_copy(slab.at[s], u_ref.at[pl.ds(0, 2 * ce), :], slab_sem.at[s]).wait()


def exchange(rows, a_msg, p_t, sizes, heads, scale):
    half = rows.shape[1:]
    n = 2 * half[1]
    hops = max(sizes) - 1
    groups = sizes[0] * sizes[1]
    ch = p_t.shape[1]
    ce = p_t.shape[0] // ch
    mine = n // groups
    k = a_msg.shape[0] * a_msg.shape[1] // SUBLANES
    return pl.pallas_call(
        functools.partial(exchange_kernel, scale),
        out_shape=(jax.ShapeDtypeStruct((heads, n, n), jnp.float32), jax.ShapeDtypeStruct((mine * ce, ch * k), jnp.bfloat16)),
        in_specs=[pl.BlockSpec(memory_space=pl.ANY), pl.BlockSpec(memory_space=pltpu.VMEM), pl.BlockSpec(memory_space=pltpu.VMEM)],
        out_specs=(pl.BlockSpec(memory_space=pltpu.VMEM), pl.BlockSpec(memory_space=pl.ANY)),
        scratch_shapes=[pltpu.VMEM(a_msg.shape, jnp.bfloat16), pltpu.VMEM((2,) + tuple(sizes) + half, jnp.bfloat16), pltpu.VMEM((half[1] // LANES, n // groups * heads, LANES), jnp.float32),
                        pltpu.VMEM((mine // 2, ch, 2 * k), jnp.bfloat16), pltpu.VMEM((k * SUBLANES, LANES), jnp.float32), pltpu.VMEM((k // LANES, mine * ch, LANES), jnp.float32),
                        pltpu.VMEM((2, 2 * ce, ch * k), jnp.bfloat16), pltpu.SemaphoreType.DMA((2,)),
                        pltpu.SemaphoreType.DMA((2,)), pltpu.SemaphoreType.DMA((8, hops)), pltpu.SemaphoreType.DMA((8, hops)),
                        pltpu.SemaphoreType.DMA((groups - 1,)), pltpu.SemaphoreType.DMA((groups - 1,))],
        compiler_params=pltpu.CompilerParams(collective_id=0, has_side_effects=True, vmem_limit_bytes=VMEM_LIMIT),
        cost_estimate=pl.CostEstimate(flops=10_000_000_000, bytes_accessed=10_000_000, transcendentals=0),
        name="exchange",
    )(rows, a_msg, p_t)


def solution(mesh):
    devices = mesh.devices
    fine = Mesh(devices.reshape(devices.shape[0], 4, 4, 4, 2), ('data', 'z', 'y', 'x', 'c'))
    seq_spec = P(('data',) + ALL_AXES)

    def per_device(msa, msa_mask, pair_act, opm_gain, opm_shift, proj_a, bias_a, proj_b, bias_b, proj_out, bias_out, row_gain, row_shift, pair_gain, pair_proj, query_w, key_w, value_w, gate_w, gate_bias, attn_out_w, attn_out_b):
        seqs, n, cm = msa.shape
        rows_dev, _, ce = pair_act.shape
        ch = proj_a.shape[1]
        groups = fine.shape['z'] * fine.shape['y']
        rows = n // groups

        a_msg, b_loc = project_ab(msa, msa_mask, opm_gain, opm_shift, proj_a, bias_a, proj_b, bias_b)
        b_all = lax.all_gather(b_loc, GROUP_AXES, axis=0, tiled=False)

        pair_in, a_msg = lax.optimization_barrier((pair_act, a_msg))
        pair_c = pair_in - jnp.mean(pair_in, axis=-1, keepdims=True)
        pair_var = jnp.mean(jnp.square(pair_c), axis=-1, keepdims=True)
        pair_n = (pair_c * lax.rsqrt(pair_var + LN_EPS) * pair_gain.astype(jnp.float32)).astype(jnp.bfloat16)
        bias_rows = jnp.einsum('ije,eh->ihj', pair_n, pair_proj, preferred_element_type=jnp.float32).astype(jnp.bfloat16)
        heads = bias_rows.shape[1]
        bias_rows = bias_rows.reshape(rows_dev, heads, 2, n // 2).transpose(2, 0, 1, 3).reshape(2, rows_dev * heads, n // 2)
        sizes = tuple(fine.shape[ax] for ax in ALL_AXES)
        near, rest_scale = split_scale(cm // heads)
        p_t = proj_out.reshape(ch, ch, ce).transpose(1, 2, 0).reshape(ch * ce, ch)
        pair_bias, u = exchange(bias_rows, a_msg, p_t, sizes, heads, 1.0 / rest_scale)

        attend = functools.partial(attention, msa, msa_mask, pair_bias, row_gain, row_shift, query_w, key_w, value_w, gate_w, gate_bias, attn_out_w, attn_out_b)
        early = seqs // 4
        msa_new = attend(0, early)

        first = lax.axis_index(GROUP_AXES) * rows
        order = lax.broadcasted_iota(jnp.int32, (rows // 2, n), 0)
        cols = lax.broadcasted_iota(jnp.int32, (rows // 2, n), 1)
        picks = [(cols == first + (order // 2) * 4 + half * 2 + order % 2).astype(jnp.bfloat16) for half in range(2)]
        picks, msa_new = lax.optimization_barrier((picks, msa_new))
        totals = []
        for half in range(2):
            part = outer_product(u, b_all, picks[half], half, ib=16)
            totals.append(lax.psum_scatter(part, SPLIT_AXES, scatter_dimension=0, tiled=True))
        msa_new, _ = lax.optimization_barrier((msa_new, part))
        msa_new = attend(early, seqs - early, msa_new)
        total = jnp.concatenate(totals, axis=0)
        outer_sum = total[:, :ce].transpose(0, 2, 1)
        counts = total[:, ce]
        pair_new = pair_act + (outer_sum + bias_out.astype(jnp.float32)) / (COUNT_EPS + counts)[:, :, None]
        return msa_new, pair_new

    in_specs = (seq_spec, seq_spec, seq_spec) + (P(),) * 19
    return jax.shard_map(per_device, mesh=fine, in_specs=in_specs, out_specs=(seq_spec, seq_spec), check_vma=False)
```

```python
import functools
import math
import jax
import jax.numpy as jnp
from jax import lax
from jax.experimental import pallas as pl
from jax.experimental.pallas import tpu as pltpu
from jax.sharding import Mesh, PartitionSpec as P

LN_EPS = 1e-5
COUNT_EPS = 1e-3
MASK_FILL = -1e9
LOG2E = math.log2(math.e)
VMEM_LIMIT = 60 * 1024 * 1024
LANES = 128
SUBLANES = 8
ALL_AXES = ('z', 'y', 'x', 'c')
GROUP_AXES = ('z', 'y')
SPLIT_AXES = ('x', 'c')


def attn_kernel(first, msa_ref, qkvg_ref, mask_ref, bias_ref, wo_ref, bo_ref, *rest):
    out_ref, w_scr, vb_scr = rest[-3:]
    n, cm = msa_ref.shape[1:]
    heads = bias_ref.shape[0]
    hd = cm // heads
    rest_scale = split_scale(hd)[1]
    lane_head = lax.broadcasted_iota(jnp.int32, (1, cm), 1) // hd
    v = qkvg_ref[0, 2]
    for h in range(heads):
        vb_scr[h * n:(h + 1) * n, :] = v * (lane_head == h).astype(jnp.bfloat16)
    keep = mask_ref[pl.ds(pl.program_id(0) + first, 1), :] > 0
    q = qkvg_ref[0, 0]
    for h in range(heads):
        qh = q * (lane_head == h).astype(jnp.bfloat16)
        s = lax.dot_general(qh, qkvg_ref[0, 1], (((1,), (1,)), ((), ())), preferred_element_type=jnp.float32)
        s = jnp.where(keep, s + bias_ref[h], MASK_FILL / rest_scale)
        m = jnp.max(s, axis=-1, keepdims=True)
        e = jnp.exp2((s - m) * (rest_scale * LOG2E))
        l = jnp.sum(e, axis=-1, keepdims=True)
        w_scr[:, h * n:(h + 1) * n] = (e * (1.0 / l)).astype(jnp.bfloat16)
    o = jnp.dot(w_scr[...], vb_scr[...], preferred_element_type=jnp.float32)
    o = (o * qkvg_ref[0, 3].astype(jnp.float32)).astype(jnp.bfloat16)
    u = jnp.dot(o, wo_ref[...], preferred_element_type=jnp.float32) + bo_ref[...].astype(jnp.float32).reshape(1, cm)
    out_ref[0] = (msa_ref[0].astype(jnp.float32) + u).astype(jnp.bfloat16)


def split_scale(hd):
    near = 2.0 ** math.floor(math.log2(hd ** -0.5))
    return near, hd ** -0.5 / near


def attention(msa, qkvg, mask, bias, wo, bo, first, count, before=None):
    s, n, cm = msa.shape
    heads = bias.shape[0]
    const = lambda shape: pl.BlockSpec(shape, lambda i: (0,) * len(shape), pipeline_mode=pl.Buffered(1))
    extra = () if before is None else (before,)
    return pl.pallas_call(
        functools.partial(attn_kernel, first),
        out_shape=jax.ShapeDtypeStruct((s, n, cm), jnp.bfloat16),
        grid=(count,),
        in_specs=[pl.BlockSpec((1, n, cm), lambda i: (i + first, 0, 0)), pl.BlockSpec((1, 4, n, cm), lambda i: (i + first, 0, 0, 0)), const((s, n)),
                  const((heads, n, n)), const((cm, cm)), const((cm,))]
                 + [pl.BlockSpec(memory_space=pl.ANY)] * len(extra),
        out_specs=pl.BlockSpec((1, n, cm), lambda i: (i + first, 0, 0)),
        scratch_shapes=[pltpu.VMEM((n, heads * n), jnp.bfloat16), pltpu.VMEM((heads * n, cm), jnp.bfloat16)],
        input_output_aliases={6: 0} if extra else {},
        compiler_params=pltpu.CompilerParams(vmem_limit_bytes=VMEM_LIMIT, dimension_semantics=("arbitrary",)),
        cost_estimate=pl.CostEstimate(flops=count * 1_500_000_000, bytes_accessed=20_000_000, transcendentals=count * 2_000_000),
        name="row_attention",
    )(msa, qkvg, mask, bias, wo, bo, *extra)


def ab_kernel(msa_ref, mask_ref, gain_ref, shift_ref, pa_ref, ba_ref, pb_ref, bb_ref, a_ref, b_ref, scr_a, scr_b):
    seqs, n, cm = msa_ref.shape
    ch = scr_b.shape[0]
    quads = n // LANES
    subs = a_ref.shape[0] // quads
    width = LANES // subs
    lane = lax.broadcasted_iota(jnp.int32, (SUBLANES, LANES), 1) // width
    w = jnp.concatenate([pa_ref[...], pb_ref[...]], axis=0)
    bias = jnp.concatenate([ba_ref[...].astype(jnp.float32).reshape(1, ch), bb_ref[...].astype(jnp.float32).reshape(1, ch)], axis=1)
    bias = jnp.broadcast_to(bias, (SUBLANES, 2 * ch)).T[:, 0:1]
    gain = gain_ref[...].astype(jnp.float32).reshape(1, cm)
    shift = shift_ref[...].astype(jnp.float32).reshape(1, cm)

    def one(s, carry):
        x = msa_ref[s].astype(jnp.float32)
        mu = jnp.mean(x, axis=-1, keepdims=True)
        xc = x - mu
        var = jnp.mean(xc * xc, axis=-1, keepdims=True)
        xn = (xc * lax.rsqrt(var + LN_EPS) * gain + shift).astype(jnp.bfloat16)
        y = lax.dot_general(w, xn, (((1,), (1,)), ((), ())), preferred_element_type=jnp.float32)
        y = (y + bias) * mask_ref[pl.ds(s, 1), :].astype(jnp.float32)
        scr_b[:, pl.ds(s, 1), :] = y[ch:2 * ch].reshape(ch, 1, n)
        for zz in range(quads):
            tiles = [y[c4 * SUBLANES:(c4 + 1) * SUBLANES, zz * LANES:(zz + 1) * LANES] for c4 in range(subs)]
            for yy in range(subs):
                out = tiles[yy]
                for c4 in range(subs):
                    if c4 != yy:
                        out = jnp.where(lane == c4, pltpu.roll(tiles[c4], ((c4 - yy) * width) % LANES, 1), out)
                scr_a[zz * subs + yy, pl.ds(pl.multiple_of(s * SUBLANES, SUBLANES), SUBLANES), :] = out
        return carry
    lax.fori_loop(0, seqs, one, 0, unroll=2)
    a_ref[...] = scr_a[...].astype(jnp.bfloat16)
    b_ref[0:ch] = scr_b[...].astype(jnp.bfloat16)
    b_ref[ch] = mask_ref[...].astype(jnp.float32).astype(jnp.bfloat16)


def project_ab(msa, mask, gain, shift, proj_a, bias_a, proj_b, bias_b):
    s, n, cm = msa.shape
    ch = proj_a.shape[1]
    return pl.pallas_call(
        ab_kernel,
        out_shape=(jax.ShapeDtypeStruct((16, s * SUBLANES, LANES), jnp.bfloat16), jax.ShapeDtypeStruct((ch + 1, s, n), jnp.bfloat16)),
        scratch_shapes=[pltpu.VMEM((16, s * SUBLANES, LANES), jnp.float32), pltpu.VMEM((ch, s, n), jnp.float32)],
        compiler_params=pltpu.CompilerParams(vmem_limit_bytes=VMEM_LIMIT),
        cost_estimate=pl.CostEstimate(flops=300_000_000, bytes_accessed=6_000_000, transcendentals=8192),
        name="project_ab",
    )(msa, mask, gain, shift, proj_a.T, bias_a, proj_b.T, bias_b)


def opm_kernel(db, ib, u_ref, b_ref, m_ref, sel_ref, out_ref):
    rows, wide, n = out_ref.shape
    ce = u_ref.shape[0] // rows
    k = m_ref.shape[0] * m_ref.shape[2]

    @pl.when(pl.program_id(0) == 0)
    def _():
        m = m_ref[...].reshape(k, n)
        mi = lax.dot_general(sel_ref[...], m, (((1,), (1,)), ((), ())), preferred_element_type=jnp.float32).astype(jnp.bfloat16)
        cnt = jnp.dot(mi, m, preferred_element_type=jnp.float32)
        for i in range(rows):
            out_ref[i, 0:ce, :] = jnp.zeros((ce, n), jnp.float32)
            out_ref[i, ce:, :] = jnp.broadcast_to(cnt[i:i + 1, :], (wide - ce, n))

    bk = jnp.concatenate([b_ref[:, dd].reshape(k, n) for dd in range(db)], axis=0)

    def block(g, carry):
        size = ib * ce
        part = jnp.dot(u_ref[pl.ds(pl.multiple_of(g * size, size), size), :], bk, preferred_element_type=jnp.float32)
        for ii in range(ib):
            out_ref[g * ib + ii, 0:ce, :] += part[ii * ce:(ii + 1) * ce]
        return carry
    lax.fori_loop(0, rows // ib, block, 0)


def outer_product(u, b_all, sel, half, db=4, ib=8):
    rows, n = sel.shape
    src, ch, s, _ = b_all.shape
    ch -= 1
    ce = u.shape[0] // (2 * rows)
    k = src * s
    return pl.pallas_call(
        functools.partial(opm_kernel, db, ib),
        out_shape=jax.ShapeDtypeStruct((rows, ce + SUBLANES, n), jnp.float32),
        grid=(ch // db,),
        in_specs=[pl.BlockSpec((rows * ce, db * k), lambda g: (half, g)),
                  pl.BlockSpec((src, db, s, n), lambda g: (0, g, 0, 0)),
                  pl.BlockSpec((src, 1, s, n), lambda g: (0, ch, 0, 0)),
                  pl.BlockSpec((rows, n), lambda g: (0, 0))],
        out_specs=pl.BlockSpec((rows, ce + SUBLANES, n), lambda g: (0, 0, 0)),
        compiler_params=pltpu.CompilerParams(vmem_limit_bytes=VMEM_LIMIT, dimension_semantics=("arbitrary",)),
        cost_estimate=pl.CostEstimate(flops=2 * rows * ce * n * k * ch, bytes_accessed=50_000_000, transcendentals=0),
        name="outer_product",
    )(u, b_all, b_all, sel)


def turn_a(ar_ref, at_ref, af, at2):
    k = af.shape[0] // SUBLANES
    rows, ch = 2 * at_ref.shape[0], at_ref.shape[1]
    af[...] = ar_ref[...].reshape(af.shape).astype(jnp.float32)
    eye = (lax.broadcasted_iota(jnp.int32, (LANES, LANES), 0) == lax.broadcasted_iota(jnp.int32, (LANES, LANES), 1)).astype(jnp.bfloat16)
    for c8 in range(SUBLANES):
        x = af[pl.ds(c8, k, stride=SUBLANES), :].astype(jnp.bfloat16)
        t = lax.dot_general(eye, x, (((1,), (1,)), ((), ())), preferred_element_type=jnp.float32)
        for c4 in range(ch // SUBLANES):
            for kk in range(k // LANES):
                at2[kk, pl.ds(c4 * SUBLANES + c8, rows, stride=ch), :] = t[c4 * rows:(c4 + 1) * rows, kk * LANES:(kk + 1) * LANES]
    for par in range(2):
        for kk in range(k // LANES):
            both = at2[kk].reshape(rows // 2, 2 * ch, LANES)[:, par * ch:(par + 1) * ch]
            at_ref[:, :, par * k + kk * LANES:par * k + (kk + 1) * LANES] = both.astype(jnp.bfloat16)


def u_rows(t, at_ref, pt_ref, slab, u_ref, sem, ce, per):
    pairs, ch, k = at_ref.shape
    k //= 2
    slot = lax.rem(t, 2)
    row = slot * pairs + (t // 2) * 2
    copy = pltpu.make_async_copy(slab.at[slot], u_ref.at[pl.ds(pl.multiple_of(row * ce, 2 * ce), 2 * ce), :], sem.at[slot])

    @pl.when(t >= 2)
    def _():
        copy.wait()

    def some(p, carry):
        u = jnp.dot(pt_ref[pl.ds(pl.multiple_of(p * per * ce, per * ce), per * ce), :], at_ref[t], preferred_element_type=jnp.float32).astype(jnp.bfloat16)
        for dd in range(per):
            for par in range(2):
                slab[slot, par * ce:(par + 1) * ce, pl.ds(pl.multiple_of((p * per + dd) * k, k), k)] = u[dd * ce:(dd + 1) * ce, par * k:(par + 1) * k]
        return carry
    lax.fori_loop(0, ch // per, some, 0)
    copy.start()


def project_rows(lo, hi, near, msa_ref, gain_ref, shift_ref, weights, gb_ref, stage, sem, out_ref):
    cm = msa_ref.shape[2]

    def one(s, carry):
        slot = lax.rem(s, 2)
        copy = pltpu.make_async_copy(stage.at[slot], out_ref.at[s], sem.at[slot])

        @pl.when(s >= 2)
        def _():
            copy.wait()
        x = msa_ref[s].astype(jnp.float32)
        mu = jnp.mean(x, axis=-1, keepdims=True)
        xc = x - mu
        var = jnp.mean(xc * xc, axis=-1, keepdims=True)
        r = (xc * lax.rsqrt(var + LN_EPS) * gain_ref[...].astype(jnp.float32).reshape(1, cm) + shift_ref[...].astype(jnp.float32).reshape(1, cm)).astype(jnp.bfloat16)
        for j, w_ref in enumerate(weights):
            y = jnp.dot(r, w_ref[...], preferred_element_type=jnp.float32)
            if j == 3:
                y = jax.nn.sigmoid(y + gb_ref[...].astype(jnp.float32).reshape(1, cm))
            y = y.astype(jnp.bfloat16)
            stage[slot, j] = y * jnp.bfloat16(near) if j == 0 else y
        copy.start()
        return carry
    lax.fori_loop(lo, hi, one, 0)


def exchange_kernel(scale, near, rows_ref, a_ref, pt_ref, msa_ref, gain_ref, shift_ref, qw_ref, kw_ref, vw_ref, gw_ref, gb_ref, out_ref, u_ref, qkvg_ref, ar_ref, bias_ref, tmp, at_ref, af, at2, slab, slab_sem, stage, stage_sem, own_sem, send_sem, recv_sem, a_send, a_recv):
    mesh_id = pl.DeviceIdType.MESH
    me = {name: lax.axis_index(name) for name in ALL_AXES}
    size = {'z': bias_ref.shape[1], 'y': bias_ref.shape[2], 'x': bias_ref.shape[3], 'c': bias_ref.shape[4]}

    def moved(name, k):
        return lax.rem(me[name] + k, size[name])

    plane = [(dz, dy) for dz in range(size['z']) for dy in range(size['y']) if dz or dy]
    barrier = pltpu.get_barrier_semaphore()
    peers = [{'z': moved('z', dz), 'y': moved('y', dy)} for dz, dy in plane]
    peers += [{'x': moved('x', k)} for k in range(1, size['x'])] + [{'c': moved('c', k)} for k in range(1, size['c'])]
    for peer in peers:
        pl.semaphore_signal(barrier, inc=1, device_id=peer, device_id_type=mesh_id)

    own = [pltpu.make_async_copy(rows_ref.at[part], bias_ref.at[part, me['z'], me['y'], me['x'], me['c']], own_sem.at[part]) for part in range(2)]
    for copy in own:
        copy.start()
    pl.semaphore_wait(barrier, len(peers))

    def spread(part, name, done, slot):
        where = tuple(pl.ds(0, size[ax]) if ax in done else me[ax] for ax in ALL_AXES)
        ref = bias_ref.at[(part,) + where]
        copies = []
        for k in range(1, size[name]):
            copies.append(pltpu.make_async_remote_copy(
                src_ref=ref, dst_ref=ref, send_sem=send_sem.at[slot, k - 1], recv_sem=recv_sem.at[slot, k - 1],
                device_id={name: moved(name, k)}, device_id_type=mesh_id))
        for copy in copies:
            copy.start()
        return copies

    orders = (('x', 'y', 'z'), ('z', 'x', 'y'))
    here = me['z'] * size['y'] + me['y']
    sends = []
    for j, (dz, dy) in enumerate(plane):
        dst = moved('z', dz) * size['y'] + moved('y', dy)
        sends.append(pltpu.make_async_remote_copy(
            src_ref=a_ref.at[dst], dst_ref=ar_ref.at[here], send_sem=a_send.at[j], recv_sem=a_recv.at[j],
            device_id={'z': moved('z', dz), 'y': moved('y', dy)}, device_id_type=mesh_id))
    for copy in sends:
        copy.start()
    ar_ref[here] = a_ref[here]
    for copy in own:
        copy.wait()
    flying = [spread(part, orders[part][0], (), part) for part in range(2)]

    def advance(phase):
        for part in range(2):
            for copy in flying[part]:
                copy.wait()
            if phase < 3:
                flying[part] = spread(part, orders[part][phase], orders[part][:phase], phase * 2 + part)
            else:
                flying[part] = spread(part, 'c', orders[part], 6 + part)

    pairs = at_ref.shape[0]
    ce = slab.shape[1] // 2

    def run(lo, hi):
        def body(t, carry):
            u_rows(t, at_ref, pt_ref, slab, u_ref, slab_sem, ce, 16)
            return carry
        lax.fori_loop(lo, hi, body, 0)

    attn_half = msa_ref.shape[0] // 2
    project_rows(0, attn_half, near, msa_ref, gain_ref, shift_ref, (qw_ref, kw_ref, vw_ref, gw_ref), gb_ref, stage, stage_sem, qkvg_ref)
    advance(1)
    project_rows(attn_half, 2 * attn_half, near, msa_ref, gain_ref, shift_ref, (qw_ref, kw_ref, vw_ref, gw_ref), gb_ref, stage, stage_sem, qkvg_ref)
    for copy in sends:
        copy.wait()
    turn_a(ar_ref, at_ref, af, at2)
    run(0, pairs // 4)
    advance(2)
    run(pairs // 4, 3 * pairs // 4)
    advance(3)
    run(3 * pairs // 4, pairs)
    heads = out_ref.shape[0]
    per = bias_ref.shape[3] * bias_ref.shape[4] * bias_ref.shape[5]
    block = per // heads
    wide = bias_ref.shape[6]
    for part in range(2):
        for copy in flying[part]:
            copy.wait()

        def place(t, carry):
            x = bias_ref[part, t // size['y'], lax.rem(t, size['y'])].reshape(per, wide).astype(jnp.float32) * scale
            for kk in range(wide // LANES):
                tmp[kk] = x[:, kk * LANES:(kk + 1) * LANES]
            for kk in range(wide // LANES):
                for h in range(heads):
                    out_ref[h, pl.ds(pl.multiple_of(t * block, block), block), part * wide + kk * LANES:part * wide + (kk + 1) * LANES] = tmp[kk, pl.ds(h, block, stride=heads), :]
            return carry
        lax.fori_loop(0, size['z'] * size['y'], place, 0)
    for s in range(2):
        pltpu.make_async_copy(stage.at[s], qkvg_ref.at[s], stage_sem.at[s]).wait()
    for s in range(2):
        pltpu.make_async_copy(slab.at[s], u_ref.at[pl.ds(0, 2 * ce), :], slab_sem.at[s]).wait()


def exchange(rows, a_msg, p_t, msa, params, sizes, heads, scale, near):
    half = rows.shape[1:]
    n = 2 * half[1]
    hops = max(sizes) - 1
    groups = sizes[0] * sizes[1]
    seqs, _, cm = msa.shape
    ch = p_t.shape[1]
    ce = p_t.shape[0] // ch
    mine = n // groups
    k = a_msg.shape[0] * a_msg.shape[1] // SUBLANES
    return pl.pallas_call(
        functools.partial(exchange_kernel, scale, near),
        out_shape=(jax.ShapeDtypeStruct((heads, n, n), jnp.float32), jax.ShapeDtypeStruct((mine * ce, ch * k), jnp.bfloat16),
                   jax.ShapeDtypeStruct((seqs, 4, n, cm), jnp.bfloat16)),
        in_specs=[pl.BlockSpec(memory_space=pl.ANY)] + [pl.BlockSpec(memory_space=pltpu.VMEM)] * (3 + len(params)),
        out_specs=(pl.BlockSpec(memory_space=pltpu.VMEM), pl.BlockSpec(memory_space=pl.ANY), pl.BlockSpec(memory_space=pl.ANY)),
        scratch_shapes=[pltpu.VMEM(a_msg.shape, jnp.bfloat16), pltpu.VMEM((2,) + tuple(sizes) + half, jnp.bfloat16), pltpu.VMEM((half[1] // LANES, n // groups * heads, LANES), jnp.float32),
                        pltpu.VMEM((mine // 2, ch, 2 * k), jnp.bfloat16), pltpu.VMEM((k * SUBLANES, LANES), jnp.float32), pltpu.VMEM((k // LANES, mine * ch, LANES), jnp.float32),
                        pltpu.VMEM((2, 2 * ce, ch * k), jnp.bfloat16), pltpu.SemaphoreType.DMA((2,)),
                        pltpu.VMEM((2, 4, n, cm), jnp.bfloat16), pltpu.SemaphoreType.DMA((2,)),
                        pltpu.SemaphoreType.DMA((2,)), pltpu.SemaphoreType.DMA((8, hops)), pltpu.SemaphoreType.DMA((8, hops)),
                        pltpu.SemaphoreType.DMA((groups - 1,)), pltpu.SemaphoreType.DMA((groups - 1,))],
        compiler_params=pltpu.CompilerParams(collective_id=0, has_side_effects=True, vmem_limit_bytes=VMEM_LIMIT),
        cost_estimate=pl.CostEstimate(flops=10_000_000_000, bytes_accessed=10_000_000, transcendentals=0),
        name="exchange",
    )(rows, a_msg, p_t, msa, *params)


def solution(mesh):
    devices = mesh.devices
    fine = Mesh(devices.reshape(devices.shape[0], 4, 4, 4, 2), ('data', 'z', 'y', 'x', 'c'))
    seq_spec = P(('data',) + ALL_AXES)

    def per_device(msa, msa_mask, pair_act, opm_gain, opm_shift, proj_a, bias_a, proj_b, bias_b, proj_out, bias_out, row_gain, row_shift, pair_gain, pair_proj, query_w, key_w, value_w, gate_w, gate_bias, attn_out_w, attn_out_b):
        seqs, n, cm = msa.shape
        rows_dev, _, ce = pair_act.shape
        ch = proj_a.shape[1]
        groups = fine.shape['z'] * fine.shape['y']
        rows = n // groups

        a_msg, b_loc = project_ab(msa, msa_mask, opm_gain, opm_shift, proj_a, bias_a, proj_b, bias_b)
        b_all = lax.all_gather(b_loc, GROUP_AXES, axis=0, tiled=False)

        pair_in, a_msg = lax.optimization_barrier((pair_act, a_msg))
        pair_c = pair_in - jnp.mean(pair_in, axis=-1, keepdims=True)
        pair_var = jnp.mean(jnp.square(pair_c), axis=-1, keepdims=True)
        pair_n = (pair_c * lax.rsqrt(pair_var + LN_EPS) * pair_gain.astype(jnp.float32)).astype(jnp.bfloat16)
        bias_rows = jnp.einsum('ije,eh->ihj', pair_n, pair_proj, preferred_element_type=jnp.float32).astype(jnp.bfloat16)
        heads = bias_rows.shape[1]
        bias_rows = bias_rows.reshape(rows_dev, heads, 2, n // 2).transpose(2, 0, 1, 3).reshape(2, rows_dev * heads, n // 2)
        sizes = tuple(fine.shape[ax] for ax in ALL_AXES)
        near, rest_scale = split_scale(cm // heads)
        p_t = proj_out.reshape(ch, ch, ce).transpose(1, 2, 0).reshape(ch * ce, ch)
        pair_bias, u, qkvg = exchange(bias_rows, a_msg, p_t, msa, (row_gain, row_shift, query_w, key_w, value_w, gate_w, gate_bias), sizes, heads, 1.0 / rest_scale, near)

        attend = functools.partial(attention, msa, qkvg, msa_mask, pair_bias, attn_out_w, attn_out_b)
        early = seqs // 4
        msa_new = attend(0, early)

        first = lax.axis_index(GROUP_AXES) * rows
        order = lax.broadcasted_iota(jnp.int32, (rows // 2, n), 0)
        cols = lax.broadcasted_iota(jnp.int32, (rows // 2, n), 1)
        picks = [(cols == first + (order // 2) * 4 + half * 2 + order % 2).astype(jnp.bfloat16) for half in range(2)]
        picks, msa_new = lax.optimization_barrier((picks, msa_new))
        totals = []
        for half in range(2):
            part = outer_product(u, b_all, picks[half], half, ib=16)
            totals.append(lax.psum_scatter(part, SPLIT_AXES, scatter_dimension=0, tiled=True))
        msa_new, _ = lax.optimization_barrier((msa_new, part))
        msa_new = attend(early, seqs - early, msa_new)
        total = jnp.concatenate(totals, axis=0)
        outer_sum = total[:, :ce].transpose(0, 2, 1)
        counts = total[:, ce]
        pair_new = pair_act + (outer_sum + bias_out.astype(jnp.float32)) / (COUNT_EPS + counts)[:, :, None]
        return msa_new, pair_new

    in_specs = (seq_spec, seq_spec, seq_spec) + (P(),) * 19
    return jax.shard_map(per_device, mesh=fine, in_specs=in_specs, out_specs=(seq_spec, seq_spec), check_vma=False)
```

```python
import functools
import math
import jax
import jax.numpy as jnp
from jax import lax
from jax.experimental import pallas as pl
from jax.experimental.pallas import tpu as pltpu
from jax.sharding import Mesh, PartitionSpec as P

LN_EPS = 1e-5
COUNT_EPS = 1e-3
MASK_FILL = -1e9
LOG2E = math.log2(math.e)
VMEM_LIMIT = 60 * 1024 * 1024
LANES = 128
SUBLANES = 8
ALL_AXES = ('z', 'y', 'x', 'c')
GROUP_AXES = ('z', 'y')
SPLIT_AXES = ('x', 'c')


def attn_kernel(first, msa_ref, mask_ref, bias_ref, gain_ref, shift_ref, qw_ref, kw_ref, vw_ref, gw_ref, gb_ref, wo_ref, bo_ref, *rest):
    out_ref, q_scr, k_scr, v_scr, g_scr, w_scr, vb_scr, b_scr = rest[-8:]
    n, cm = msa_ref.shape[1:]
    heads = bias_ref.shape[0]
    hd = cm // heads
    near, rest_scale = split_scale(hd)

    @pl.when(pl.program_id(0) == 0)
    def _():
        for h in range(heads):
            b_scr[h] = bias_ref[h].astype(jnp.float32) * (1.0 / rest_scale)

    x = msa_ref[0].astype(jnp.float32)
    mu = jnp.mean(x, axis=-1, keepdims=True)
    xc = x - mu
    var = jnp.mean(xc * xc, axis=-1, keepdims=True)
    r = (xc * lax.rsqrt(var + LN_EPS) * gain_ref[...].astype(jnp.float32).reshape(1, cm) + shift_ref[...].astype(jnp.float32).reshape(1, cm)).astype(jnp.bfloat16)
    q_scr[...] = jnp.dot(r, qw_ref[...], preferred_element_type=jnp.float32).astype(jnp.bfloat16) * jnp.bfloat16(near)
    k_scr[...] = jnp.dot(r, kw_ref[...], preferred_element_type=jnp.float32).astype(jnp.bfloat16)
    v = jnp.dot(r, vw_ref[...], preferred_element_type=jnp.float32).astype(jnp.bfloat16)
    g_scr[...] = jax.nn.sigmoid(jnp.dot(r, gw_ref[...], preferred_element_type=jnp.float32) + gb_ref[...].astype(jnp.float32).reshape(1, cm)).astype(jnp.bfloat16)
    lane_head = lax.broadcasted_iota(jnp.int32, (1, cm), 1) // hd
    for h in range(heads):
        vb_scr[h * n:(h + 1) * n, :] = v * (lane_head == h).astype(jnp.bfloat16)
    keep = mask_ref[pl.ds(pl.program_id(0) + first, 1), :] > 0
    q = q_scr[...]
    for h in range(heads):
        qh = q * (lane_head == h).astype(jnp.bfloat16)
        s = lax.dot_general(qh, k_scr[...], (((1,), (1,)), ((), ())), preferred_element_type=jnp.float32)
        s = jnp.where(keep, s + b_scr[h], MASK_FILL / rest_scale)
        m = jnp.max(s, axis=-1, keepdims=True)
        e = jnp.exp2((s - m) * (rest_scale * LOG2E))
        l = jnp.sum(e, axis=-1, keepdims=True)
        w_scr[:, h * n:(h + 1) * n] = (e * (1.0 / l)).astype(jnp.bfloat16)
    o = jnp.dot(w_scr[...], vb_scr[...], preferred_element_type=jnp.float32)
    o = (o * g_scr[...].astype(jnp.float32)).astype(jnp.bfloat16)
    u = jnp.dot(o, wo_ref[...], preferred_element_type=jnp.float32) + bo_ref[...].astype(jnp.float32).reshape(1, cm)
    out_ref[0] = (msa_ref[0].astype(jnp.float32) + u).astype(jnp.bfloat16)


def split_scale(hd):
    near = 2.0 ** math.floor(math.log2(hd ** -0.5))
    return near, hd ** -0.5 / near


def attention(msa, mask, bias, gain, shift, qw, kw, vw, gw, gb, wo, bo, first, count, before=None):
    s, n, cm = msa.shape
    heads = bias.shape[0]
    const = lambda shape: pl.BlockSpec(shape, lambda i: (0,) * len(shape), pipeline_mode=pl.Buffered(1))
    extra = () if before is None else (before,)
    return pl.pallas_call(
        functools.partial(attn_kernel, first),
        out_shape=jax.ShapeDtypeStruct((s, n, cm), jnp.bfloat16),
        grid=(count,),
        in_specs=[pl.BlockSpec((1, n, cm), lambda i: (i + first, 0, 0)), const((s, n)),
                  const((heads, n, n)), const((cm,)), const((cm,)), const((cm, cm)), const((cm, cm)), const((cm, cm)), const((cm, cm)), const((cm,)), const((cm, cm)), const((cm,))]
                 + [pl.BlockSpec(memory_space=pl.ANY)] * len(extra),
        out_specs=pl.BlockSpec((1, n, cm), lambda i: (i + first, 0, 0)),
        scratch_shapes=[pltpu.VMEM((n, cm), jnp.bfloat16)] * 4 + [pltpu.VMEM((n, heads * n), jnp.bfloat16), pltpu.VMEM((heads * n, cm), jnp.bfloat16), pltpu.VMEM((heads, n, n), jnp.float32)],
        input_output_aliases={12: 0} if extra else {},
        compiler_params=pltpu.CompilerParams(vmem_limit_bytes=VMEM_LIMIT, dimension_semantics=("arbitrary",)),
        cost_estimate=pl.CostEstimate(flops=count * 1_500_000_000, bytes_accessed=20_000_000, transcendentals=count * 2_000_000),
        name="row_attention",
    )(msa, mask, bias, gain, shift, qw, kw, vw, gw, gb, wo, bo, *extra)


def ab_kernel(msa_ref, mask_ref, gain_ref, shift_ref, pa_ref, ba_ref, pb_ref, bb_ref, a_ref, b_ref, scr_a, scr_b):
    seqs, n, cm = msa_ref.shape
    ch = scr_b.shape[0]
    quads = n // LANES
    subs = a_ref.shape[0] // quads
    width = LANES // subs
    lane = lax.broadcasted_iota(jnp.int32, (SUBLANES, LANES), 1) // width
    w = jnp.concatenate([pa_ref[...], pb_ref[...]], axis=0)
    bias = jnp.concatenate([ba_ref[...].astype(jnp.float32).reshape(1, ch), bb_ref[...].astype(jnp.float32).reshape(1, ch)], axis=1)
    bias = jnp.broadcast_to(bias, (SUBLANES, 2 * ch)).T[:, 0:1]
    gain = gain_ref[...].astype(jnp.float32).reshape(1, cm)
    shift = shift_ref[...].astype(jnp.float32).reshape(1, cm)

    def one(s, carry):
        x = msa_ref[s].astype(jnp.float32)
        mu = jnp.mean(x, axis=-1, keepdims=True)
        xc = x - mu
        var = jnp.mean(xc * xc, axis=-1, keepdims=True)
        xn = (xc * lax.rsqrt(var + LN_EPS) * gain + shift).astype(jnp.bfloat16)
        y = lax.dot_general(w, xn, (((1,), (1,)), ((), ())), preferred_element_type=jnp.float32)
        y = (y + bias) * mask_ref[pl.ds(s, 1), :].astype(jnp.float32)
        scr_b[:, pl.ds(s, 1), :] = y[ch:2 * ch].reshape(ch, 1, n)
        for zz in range(quads):
            tiles = [y[c4 * SUBLANES:(c4 + 1) * SUBLANES, zz * LANES:(zz + 1) * LANES] for c4 in range(subs)]
            for yy in range(subs):
                out = tiles[yy]
                for c4 in range(subs):
                    if c4 != yy:
                        out = jnp.where(lane == c4, pltpu.roll(tiles[c4], ((c4 - yy) * width) % LANES, 1), out)
                scr_a[zz * subs + yy, pl.ds(pl.multiple_of(s * SUBLANES, SUBLANES), SUBLANES), :] = out
        return carry
    lax.fori_loop(0, seqs, one, 0, unroll=2)
    a_ref[...] = scr_a[...].astype(jnp.bfloat16)
    b_ref[0:ch] = scr_b[...].astype(jnp.bfloat16)
    b_ref[ch] = mask_ref[...].astype(jnp.float32).astype(jnp.bfloat16)


def project_ab(msa, mask, gain, shift, proj_a, bias_a, proj_b, bias_b):
    s, n, cm = msa.shape
    ch = proj_a.shape[1]
    return pl.pallas_call(
        ab_kernel,
        out_shape=(jax.ShapeDtypeStruct((16, s * SUBLANES, LANES), jnp.bfloat16), jax.ShapeDtypeStruct((ch + 1, s, n), jnp.bfloat16)),
        scratch_shapes=[pltpu.VMEM((16, s * SUBLANES, LANES), jnp.float32), pltpu.VMEM((ch, s, n), jnp.float32)],
        compiler_params=pltpu.CompilerParams(vmem_limit_bytes=VMEM_LIMIT),
        cost_estimate=pl.CostEstimate(flops=300_000_000, bytes_accessed=6_000_000, transcendentals=8192),
        name="project_ab",
    )(msa, mask, gain, shift, proj_a.T, bias_a, proj_b.T, bias_b)


def opm_kernel(db, ib, u_ref, b_ref, m_ref, sel_ref, out_ref):
    rows, wide, n = out_ref.shape
    ce = u_ref.shape[0] // rows
    k = m_ref.shape[0] * m_ref.shape[2]

    @pl.when(pl.program_id(0) == 0)
    def _():
        m = m_ref[...].reshape(k, n)
        mi = lax.dot_general(sel_ref[...], m, (((1,), (1,)), ((), ())), preferred_element_type=jnp.float32).astype(jnp.bfloat16)
        cnt = jnp.dot(mi, m, preferred_element_type=jnp.float32)
        for i in range(rows):
            out_ref[i, 0:ce, :] = jnp.zeros((ce, n), jnp.float32)
            out_ref[i, ce:, :] = jnp.broadcast_to(cnt[i:i + 1, :], (wide - ce, n))

    bk = jnp.concatenate([b_ref[:, dd].reshape(k, n) for dd in range(db)], axis=0)

    def block(g, carry):
        size = ib * ce
        part = jnp.dot(u_ref[pl.ds(pl.multiple_of(g * size, size), size), :], bk, preferred_element_type=jnp.float32)
        for ii in range(ib):
            out_ref[g * ib + ii, 0:ce, :] += part[ii * ce:(ii + 1) * ce]
        return carry
    lax.fori_loop(0, rows // ib, block, 0)


def outer_product(u, b_all, sel, half, db=4, ib=8):
    rows, n = sel.shape
    src, ch, s, _ = b_all.shape
    ch -= 1
    ce = u.shape[0] // (2 * rows)
    k = src * s
    return pl.pallas_call(
        functools.partial(opm_kernel, db, ib),
        out_shape=jax.ShapeDtypeStruct((rows, ce + SUBLANES, n), jnp.float32),
        grid=(ch // db,),
        in_specs=[pl.BlockSpec((rows * ce, db * k), lambda g: (half, g)),
                  pl.BlockSpec((src, db, s, n), lambda g: (0, g, 0, 0)),
                  pl.BlockSpec((src, 1, s, n), lambda g: (0, ch, 0, 0)),
                  pl.BlockSpec((rows, n), lambda g: (0, 0))],
        out_specs=pl.BlockSpec((rows, ce + SUBLANES, n), lambda g: (0, 0, 0)),
        compiler_params=pltpu.CompilerParams(vmem_limit_bytes=VMEM_LIMIT, dimension_semantics=("arbitrary",)),
        cost_estimate=pl.CostEstimate(flops=2 * rows * ce * n * k * ch, bytes_accessed=50_000_000, transcendentals=0),
        name="outer_product",
    )(u, b_all, b_all, sel)


def turn_a(ar_ref, at_ref, af, at2):
    k = af.shape[0] // SUBLANES
    rows, ch = 2 * at_ref.shape[0], at_ref.shape[1]
    af[...] = ar_ref[...].reshape(af.shape).astype(jnp.float32)
    eye = (lax.broadcasted_iota(jnp.int32, (LANES, LANES), 0) == lax.broadcasted_iota(jnp.int32, (LANES, LANES), 1)).astype(jnp.bfloat16)
    for c8 in range(SUBLANES):
        x = af[pl.ds(c8, k, stride=SUBLANES), :].astype(jnp.bfloat16)
        t = lax.dot_general(eye, x, (((1,), (1,)), ((), ())), preferred_element_type=jnp.float32)
        for c4 in range(ch // SUBLANES):
            for kk in range(k // LANES):
                at2[kk, pl.ds(c4 * SUBLANES + c8, rows, stride=ch), :] = t[c4 * rows:(c4 + 1) * rows, kk * LANES:(kk + 1) * LANES]
    for par in range(2):
        for kk in range(k // LANES):
            both = at2[kk].reshape(rows // 2, 2 * ch, LANES)[:, par * ch:(par + 1) * ch]
            at_ref[:, :, par * k + kk * LANES:par * k + (kk + 1) * LANES] = both.astype(jnp.bfloat16)


def u_rows(t, at_ref, pt_ref, slab, u_ref, sem, ce, per):
    pairs, ch, k = at_ref.shape
    k //= 2
    slot = lax.rem(t, 2)
    row = slot * pairs + (t // 2) * 2
    copy = pltpu.make_async_copy(slab.at[slot], u_ref.at[pl.ds(pl.multiple_of(row * ce, 2 * ce), 2 * ce), :], sem.at[slot])

    @pl.when(t >= 2)
    def _():
        copy.wait()

    def some(p, carry):
        u = jnp.dot(pt_ref[pl.ds(pl.multiple_of(p * per * ce, per * ce), per * ce), :], at_ref[t], preferred_element_type=jnp.float32).astype(jnp.bfloat16)
        for dd in range(per):
            for par in range(2):
                slab[slot, par * ce:(par + 1) * ce, pl.ds(pl.multiple_of((p * per + dd) * k, k), k)] = u[dd * ce:(dd + 1) * ce, par * k:(par + 1) * k]
        return carry
    lax.fori_loop(0, ch // per, some, 0)
    copy.start()


def exchange_kernel(rows_ref, a_ref, pt_ref, out_ref, u_ref, ar_ref, bias_ref, tmp, at_ref, af, at2, slab, slab_sem, own_sem, send_sem, recv_sem, a_send, a_recv):
    mesh_id = pl.DeviceIdType.MESH
    me = {name: lax.axis_index(name) for name in ALL_AXES}
    size = {'z': bias_ref.shape[1], 'y': bias_ref.shape[2], 'x': bias_ref.shape[3], 'c': bias_ref.shape[4]}

    def moved(name, k):
        return lax.rem(me[name] + k, size[name])

    plane = [(dz, dy) for dz in range(size['z']) for dy in range(size['y']) if dz or dy]
    barrier = pltpu.get_barrier_semaphore()
    peers = [{'z': moved('z', dz), 'y': moved('y', dy)} for dz, dy in plane]
    peers += [{'x': moved('x', k)} for k in range(1, size['x'])] + [{'c': moved('c', k)} for k in range(1, size['c'])]
    for peer in peers:
        pl.semaphore_signal(barrier, inc=1, device_id=peer, device_id_type=mesh_id)

    own = [pltpu.make_async_copy(rows_ref.at[part], bias_ref.at[part, me['z'], me['y'], me['x'], me['c']], own_sem.at[part]) for part in range(2)]
    for copy in own:
        copy.start()
    pl.semaphore_wait(barrier, len(peers))

    def spread(part, name, done, slot):
        where = tuple(pl.ds(0, size[ax]) if ax in done else me[ax] for ax in ALL_AXES)
        ref = bias_ref.at[(part,) + where]
        copies = []
        for k in range(1, size[name]):
            copies.append(pltpu.make_async_remote_copy(
                src_ref=ref, dst_ref=ref, send_sem=send_sem.at[slot, k - 1], recv_sem=recv_sem.at[slot, k - 1],
                device_id={name: moved(name, k)}, device_id_type=mesh_id))
        for copy in copies:
            copy.start()
        return copies

    orders = (('x', 'y', 'z'), ('z', 'x', 'y'))
    here = me['z'] * size['y'] + me['y']
    sends = []
    for j, (dz, dy) in enumerate(plane):
        dst = moved('z', dz) * size['y'] + moved('y', dy)
        sends.append(pltpu.make_async_remote_copy(
            src_ref=a_ref.at[dst], dst_ref=ar_ref.at[here], send_sem=a_send.at[j], recv_sem=a_recv.at[j],
            device_id={'z': moved('z', dz), 'y': moved('y', dy)}, device_id_type=mesh_id))
    for copy in sends:
        copy.start()
    ar_ref[here] = a_ref[here]
    for copy in own:
        copy.wait()
    flying = [spread(part, orders[part][0], (), part) for part in range(2)]

    def advance(phase):
        for part in range(2):
            for copy in flying[part]:
                copy.wait()
            if phase < 3:
                flying[part] = spread(part, orders[part][phase], orders[part][:phase], phase * 2 + part)
            else:
                flying[part] = spread(part, 'c', orders[part], 6 + part)

    pairs = at_ref.shape[0]
    ce = slab.shape[1] // 2

    def run(lo, hi):
        def body(t, carry):
            u_rows(t, at_ref, pt_ref, slab, u_ref, slab_sem, ce, 16)
            return carry
        lax.fori_loop(lo, hi, body, 0)

    for copy in sends:
        copy.wait()
    advance(1)
    turn_a(ar_ref, at_ref, af, at2)
    run(0, pairs // 4)
    advance(2)
    run(pairs // 4, 3 * pairs // 4)
    advance(3)
    run(3 * pairs // 4, pairs)
    heads = out_ref.shape[0]
    per = bias_ref.shape[3] * bias_ref.shape[4] * bias_ref.shape[5]
    block = per // heads
    wide = bias_ref.shape[6]
    for part in range(2):
        for copy in flying[part]:
            copy.wait()

        def place(t, carry):
            x = bias_ref[part, t // size['y'], lax.rem(t, size['y'])].reshape(per, wide).astype(jnp.float32)
            for kk in range(wide // LANES):
                tmp[kk] = x[:, kk * LANES:(kk + 1) * LANES]
            for kk in range(wide // LANES):
                for h in range(heads):
                    out_ref[h, pl.ds(pl.multiple_of(t * block, block), block), part * wide + kk * LANES:part * wide + (kk + 1) * LANES] = tmp[kk, pl.ds(h, block, stride=heads), :].astype(jnp.bfloat16)
            return carry
        lax.fori_loop(0, size['z'] * size['y'], place, 0)
    for s in range(2):
        pltpu.make_async_copy(slab.at[s], u_ref.at[pl.ds(0, 2 * ce), :], slab_sem.at[s]).wait()


def exchange(rows, a_msg, p_t, sizes, heads):
    half = rows.shape[1:]
    n = 2 * half[1]
    hops = max(sizes) - 1
    groups = sizes[0] * sizes[1]
    ch = p_t.shape[1]
    ce = p_t.shape[0] // ch
    mine = n // groups
    k = a_msg.shape[0] * a_msg.shape[1] // SUBLANES
    return pl.pallas_call(
        exchange_kernel,
        out_shape=(jax.ShapeDtypeStruct((heads, n, n), jnp.bfloat16), jax.ShapeDtypeStruct((mine * ce, ch * k), jnp.bfloat16)),
        in_specs=[pl.BlockSpec(memory_space=pl.ANY), pl.BlockSpec(memory_space=pltpu.VMEM), pl.BlockSpec(memory_space=pltpu.VMEM)],
        out_specs=(pl.BlockSpec(memory_space=pltpu.VMEM), pl.BlockSpec(memory_space=pl.ANY)),
        scratch_shapes=[pltpu.VMEM(a_msg.shape, jnp.bfloat16), pltpu.VMEM((2,) + tuple(sizes) + half, jnp.bfloat16), pltpu.VMEM((half[1] // LANES, n // groups * heads, LANES), jnp.float32),
                        pltpu.VMEM((mine // 2, ch, 2 * k), jnp.bfloat16), pltpu.VMEM((k * SUBLANES, LANES), jnp.float32), pltpu.VMEM((k // LANES, mine * ch, LANES), jnp.float32),
                        pltpu.VMEM((2, 2 * ce, ch * k), jnp.bfloat16), pltpu.SemaphoreType.DMA((2,)),
                        pltpu.SemaphoreType.DMA((2,)), pltpu.SemaphoreType.DMA((8, hops)), pltpu.SemaphoreType.DMA((8, hops)),
                        pltpu.SemaphoreType.DMA((groups - 1,)), pltpu.SemaphoreType.DMA((groups - 1,))],
        compiler_params=pltpu.CompilerParams(collective_id=0, has_side_effects=True, vmem_limit_bytes=VMEM_LIMIT),
        cost_estimate=pl.CostEstimate(flops=10_000_000_000, bytes_accessed=10_000_000, transcendentals=0),
        name="exchange",
    )(rows, a_msg, p_t)


def pair_kernel(low_ref, high_ref, pair_ref, bias_ref, out_ref):
    rows, n, ce = pair_ref.shape
    bias = jnp.broadcast_to(bias_ref[...].astype(jnp.float32).reshape(1, ce), (SUBLANES, ce)).T[:, 0:1]
    for r in range(rows):
        t_ref = low_ref if r < rows // 2 else high_ref
        t = t_ref[r % (rows // 2)]
        val = (t[0:ce] + bias) / (COUNT_EPS + t[ce:ce + 1])
        out_ref[r] = pair_ref[r] + val.T


def finish_pair(low, high, pair_act, bias_out):
    return pl.pallas_call(
        pair_kernel,
        out_shape=jax.ShapeDtypeStruct(pair_act.shape, jnp.float32),
        cost_estimate=pl.CostEstimate(flops=2_000_000, bytes_accessed=4_000_000, transcendentals=0),
        name="finish_pair",
    )(low, high, pair_act, bias_out)


def solution(mesh):
    devices = mesh.devices
    fine = Mesh(devices.reshape(devices.shape[0], 4, 4, 4, 2), ('data', 'z', 'y', 'x', 'c'))
    seq_spec = P(('data',) + ALL_AXES)

    def per_device(msa, msa_mask, pair_act, opm_gain, opm_shift, proj_a, bias_a, proj_b, bias_b, proj_out, bias_out, row_gain, row_shift, pair_gain, pair_proj, query_w, key_w, value_w, gate_w, gate_bias, attn_out_w, attn_out_b):
        seqs, n, cm = msa.shape
        rows_dev, _, ce = pair_act.shape
        ch = proj_a.shape[1]
        groups = fine.shape['z'] * fine.shape['y']
        rows = n // groups

        a_msg, b_loc = project_ab(msa, msa_mask, opm_gain, opm_shift, proj_a, bias_a, proj_b, bias_b)
        b_all = lax.all_gather(b_loc, GROUP_AXES, axis=0, tiled=False)

        pair_in, a_msg = lax.optimization_barrier((pair_act, a_msg))
        pair_c = pair_in - jnp.mean(pair_in, axis=-1, keepdims=True)
        pair_var = jnp.mean(jnp.square(pair_c), axis=-1, keepdims=True)
        pair_n = (pair_c * lax.rsqrt(pair_var + LN_EPS) * pair_gain.astype(jnp.float32)).astype(jnp.bfloat16)
        bias_rows = jnp.einsum('ije,eh->ihj', pair_n, pair_proj, preferred_element_type=jnp.float32).astype(jnp.bfloat16)
        heads = bias_rows.shape[1]
        bias_rows = bias_rows.reshape(rows_dev, heads, 2, n // 2).transpose(2, 0, 1, 3).reshape(2, rows_dev * heads, n // 2)
        sizes = tuple(fine.shape[ax] for ax in ALL_AXES)
        p_t = proj_out.reshape(ch, ch, ce).transpose(1, 2, 0).reshape(ch * ce, ch)
        pair_bias, u = exchange(bias_rows, a_msg, p_t, sizes, heads)

        attend = functools.partial(attention, msa, msa_mask, pair_bias, row_gain, row_shift, query_w, key_w, value_w, gate_w, gate_bias, attn_out_w, attn_out_b)
        early = seqs // 4
        msa_new = attend(0, early)

        first = lax.axis_index(GROUP_AXES) * rows
        order = lax.broadcasted_iota(jnp.int32, (rows // 2, n), 0)
        cols = lax.broadcasted_iota(jnp.int32, (rows // 2, n), 1)
        picks = [(cols == first + (order // 2) * 4 + half * 2 + order % 2).astype(jnp.bfloat16) for half in range(2)]
        picks, msa_new = lax.optimization_barrier((picks, msa_new))
        totals = []
        for half in range(2):
            part = outer_product(u, b_all, picks[half], half, ib=16)
            totals.append(lax.psum_scatter(part, SPLIT_AXES, scatter_dimension=0, tiled=True))
        msa_new, _ = lax.optimization_barrier((msa_new, part))
        msa_new = attend(early, seqs - early, msa_new)
        pair_new = finish_pair(totals[0], totals[1], pair_act, bias_out)
        return msa_new, pair_new

    in_specs = (seq_spec, seq_spec, seq_spec) + (P(),) * 19
    return jax.shard_map(per_device, mesh=fine, in_specs=in_specs, out_specs=(seq_spec, seq_spec), check_vma=False)
```
